64 devices in a mesh: rep: 4 (over x, y), dp: 16 (over z, core).
Axes of the slice: x: 2, y: 2, z: 8, core: 2. Of those that a mesh axis runs over, the one named last changes fastest.
The devices are a block of a 4x4x8 slice.
Arguments:
- x: bfloat16 [64, 2048, 640], P(('rep', 'dp')), parts along dimension 0
- dy: bfloat16 [64, 2048, 640], P(('rep', 'dp')), parts along dimension 0
- w_gate: bfloat16 [2, 640, 2048], replicated
- w_up: bfloat16 [2, 640, 2048], replicated
- w_down: bfloat16 [2, 2048, 640], replicated
- m_w_gate: float32 [2, 640, 2048], P(None, 'dp')
- m_w_up: float32 [2, 640, 2048], P(None, 'dp')
- m_w_down: float32 [2, 2048, 640], P(None, 'dp')
- v_w_gate: float32 [2, 640, 2048], P(None, 'dp')
- v_w_up: float32 [2, 640, 2048], P(None, 'dp')
- v_w_down: float32 [2, 2048, 640], P(None, 'dp')
Outputs:
- output 1: bfloat16 [8, 640, 2048], P('rep'), parts along dimension 0
- output 2: bfloat16 [8, 640, 2048], P('rep'), parts along dimension 0
- output 3: bfloat16 [8, 2048, 640], P('rep'), parts along dimension 0
- output 4: float32 [8, 640, 2048], P('rep', 'dp'), parts along dimension 0
- output 5: float32 [8, 640, 2048], P('rep', 'dp'), parts along dimension 0
- output 6: float32 [8, 2048, 640], P('rep', 'dp'), parts along dimension 0
- output 7: float32 [8, 640, 2048], P('rep', 'dp'), parts along dimension 0
- output 8: float32 [8, 640, 2048], P('rep', 'dp'), parts along dimension 0
- output 9: float32 [8, 2048, 640], P('rep', 'dp'), parts along dimension 0
There are 4 independent parts. The reference program is written for one: setup_inputs(seed, part) draws one part's arguments, and reference() takes and returns one part's arrays. A program takes and returns all parts, laid end to end along the dimension named above; an argument that names none is the same for every part.
All inputs are finite; a program needn't handle non-finite values.
Results may differ from the reference program's by a relative error of at most 0.022.
Values are sent between devices in bfloat16 or wider.
A program may use at most 768 MiB of HBM per device.

```python
import jax
import jax.numpy as jnp
from jax import lax

SEQUENCES = 16
TOKENS = 2048
D = 640
FF = 2048
LAYERS = 2
NAMES = ("w_gate", "w_up", "w_down")
SHAPES = {"w_gate": (LAYERS, D, FF), "w_up": (LAYERS, D, FF), "w_down": (LAYERS, FF, D)}


def bump(key, n, height):
    away = (jnp.arange(n, dtype=jnp.int32) - jax.random.randint(key, (), 0, n, jnp.int32)) % n
    return jnp.where(away < n // 8, height, 1.0)


def together(key, own, strength):
    shared = jax.random.normal(key, own.shape[1:], jnp.float32)
    return (own + strength * shared) * lax.rsqrt(1 + strength * strength)


def setup_inputs(seed: int = 0, part: int = 0) -> dict:
    kx, kdy, ka, kb, kz, kf, kh, kl, *keys = jax.random.split(jax.random.key(seed), 8 + 3 * len(NAMES))
    kx, kdy, ka, kb = (jax.random.fold_in(k, part) for k in (kx, kdy, ka, kb))
    kw, km, kv = (keys[i::3] for i in range(3))
    shape = (SEQUENCES, TOKENS, D)
    much_x, much_dy = jax.random.uniform(kz, (2,), jnp.float32, 0.0, 1.0)
    loud = 2.0 ** jax.random.uniform(jax.random.fold_in(kz, 1), (), jnp.float32, -1.0, 2.0)
    layers = 2.0 ** jax.random.uniform(kl, (LAYERS, 1, 1), jnp.float32, -1.0, 1.0)
    x = together(ka, jax.random.normal(kx, shape, jnp.float32), much_x) * bump(kf, D, 4.0)
    dy = together(kb, jax.random.normal(kdy, shape, jnp.float32), much_dy)
    drawn = {"x": x.astype(jnp.bfloat16), "dy": (loud * dy * (SEQUENCES * TOKENS) ** -0.5).astype(jnp.bfloat16)}
    for key, name in zip(kw, NAMES, strict=True):
        w = jax.random.normal(key, SHAPES[name], jnp.float32) * SHAPES[name][1] ** -0.5
        drawn[name] = (w * {"w_gate": 1.0, "w_up": bump(kh, FF, 4.0), "w_down": layers}[name]).astype(jnp.bfloat16)
    for key, name in zip(km, NAMES, strict=True):
        drawn[f"m_{name}"] = 0.1 * jax.random.normal(key, SHAPES[name], jnp.float32)
    for key, name in zip(kv, NAMES, strict=True):
        drawn[f"v_{name}"] = jax.random.uniform(key, SHAPES[name], jnp.float32, 0.005, 0.015)
    return drawn


def matmul(a, w):
    return jnp.dot(a, w, preferred_element_type=jnp.float32).astype(jnp.bfloat16)


def normed(h):
    wide = h.astype(jnp.float32)
    scale = lax.rsqrt(jnp.mean(wide**2, -1, keepdims=True) + 1e-6)
    return (wide * scale).astype(jnp.bfloat16)


def layer(h, w):
    a = normed(h)
    gate = jnp.dot(a, w["w_gate"], preferred_element_type=jnp.float32)
    up = jnp.dot(a, w["w_up"], preferred_element_type=jnp.float32)
    return h + matmul((jax.nn.silu(gate) * up).astype(jnp.bfloat16), w["w_down"])


def adamw(w, m, v, g):
    m = 0.9 * m + 0.1 * g
    v = 0.95 * v + 0.05 * g * g
    step = m * lax.rsqrt(v + 1e-8) + 0.1 * w
    return (w - 0.02 * step).astype(jnp.bfloat16), m, v


def stack(weights, h):
    return lax.scan(lambda h, w: (layer(h, w), None), h, weights)[0]


def reference(x, dy, w_gate, w_up, w_down, m_w_gate, m_w_up, m_w_down, v_w_gate, v_w_up, v_w_down):
    weights = dict(zip(NAMES, (w_gate, w_up, w_down), strict=True))

    def take(so_far, sequence):
        h, by_y = sequence
        _, back = jax.vjp(lambda w: stack(w, h), weights)
        return jax.tree.map(lambda total, term: total + term.astype(jnp.float32), so_far, back(by_y)[0]), None

    none_yet = {name: jnp.zeros(w.shape, jnp.float32) for name, w in weights.items()}
    by_weights, _ = lax.scan(take, none_yet, (x, dy))
    gradients = [by_weights[name].astype(jnp.bfloat16).astype(jnp.float32) for name in NAMES]
    new = [
        adamw(w.astype(jnp.float32), m, v, g)
        for w, m, v, g in zip((w_gate, w_up, w_down), (m_w_gate, m_w_up, m_w_down), (v_w_gate, v_w_up, v_w_down), gradients, strict=True)
    ]
    return tuple(one[which] for which in range(3) for one in new)
```

```python
import jax
import jax.numpy as jnp
from jax import lax
from jax.sharding import PartitionSpec as P

NAMES = ("w_gate", "w_up", "w_down")


def matmul(a, w):
    return jnp.dot(a, w, preferred_element_type=jnp.float32).astype(jnp.bfloat16)


def normed(h):
    wide = h.astype(jnp.float32)
    scale = lax.rsqrt(jnp.mean(wide**2, -1, keepdims=True) + 1e-6)
    return (wide * scale).astype(jnp.bfloat16)


def layer(h, w):
    a = normed(h)
    gate = jnp.dot(a, w["w_gate"], preferred_element_type=jnp.float32)
    up = jnp.dot(a, w["w_up"], preferred_element_type=jnp.float32)
    return h + matmul((jax.nn.silu(gate) * up).astype(jnp.bfloat16), w["w_down"])


def adamw(w, m, v, g):
    m = 0.9 * m + 0.1 * g
    v = 0.95 * v + 0.05 * g * g
    step = m * lax.rsqrt(v + 1e-8) + 0.1 * w
    return (w - 0.02 * step).astype(jnp.bfloat16), m, v


def solution(mesh):
    size = mesh.shape["dp"]

    def body(x, dy, *arrays):
        weights, m, v = (arrays[i : i + 3] for i in (0, 3, 6))
        layers = weights[0].shape[0]
        per_layer = [{name: w[n] for name, w in zip(NAMES, weights)} for n in range(layers)]

        def stack(per_layer):
            h = x[0]
            for w in per_layer:
                h = layer(h, w)
            return h

        _, back = jax.vjp(stack, per_layer)
        grads = back(dy[0])[0]
        me = lax.axis_index("dp")
        new = {}
        for n in reversed(range(layers)):
            for i, name in enumerate(NAMES):
                g = lax.psum_scatter(grads[n][name], "dp", scatter_dimension=0, tiled=True)
                rows = g.shape[0]
                mine = lax.dynamic_slice_in_dim(weights[i][n], me * rows, rows)
                w1, m1, v1 = adamw(mine.astype(jnp.float32), m[i][n], v[i][n], g.astype(jnp.float32))
                new[n, i] = lax.all_gather(w1, "dp", axis=0, tiled=True), m1, v1
        return tuple(jnp.stack([new[n, i][k] for n in range(layers)]) for k in range(3) for i in range(3))

    seq, whole, rows = P(("rep", "dp"), None, None), P(None, None, None), P(None, "dp", None)
    return jax.shard_map(
        body,
        mesh=mesh,
        in_specs=(seq, seq, whole, whole, whole) + (rows,) * 6,
        out_specs=(P("rep", None, None),) * 3 + (P("rep", "dp", None),) * 6,
        check_vma=False,
    )
```

```python
import functools

import jax
import jax.numpy as jnp
from jax import lax
from jax.experimental import pallas as pl
from jax.experimental.pallas import tpu as pltpu
from jax.sharding import PartitionSpec as P

MESH = pl.DeviceIdType.MESH
BF, F32 = jnp.bfloat16, jnp.float32
BLOCK = 256
STRIPS = 4
POINTS = 3
ANY = pl.BlockSpec(memory_space=pl.ANY)


def dot(a, b, dims=((1,), (0,))):
    return lax.dot_general(a, b, (dims, ((), ())), preferred_element_type=F32)


def scale_of(wide):
    return lax.rsqrt(jnp.mean(wide * wide, -1, keepdims=True) + 1e-6)


def forward(x_ref, dy_ref, wg_ref, wu_ref, wd_ref, a_ref, at_ref, h_ref, b_ref, bt_ref, dyt_ref, act_ref):
    wide = x_ref[...].astype(F32)
    a = wide * scale_of(wide)
    at_ref[...] = a.T.astype(BF)
    a = a.astype(BF)
    a_ref[...] = a
    width = wg_ref.shape[1] // STRIPS
    for j in range(STRIPS):
        cols = slice(j * width, (j + 1) * width)
        gate, up = dot(a, wg_ref[:, cols]), dot(a, wu_ref[:, cols])
        act_ref[:, cols] = (gate * jax.nn.sigmoid(gate) * up).astype(BF)
    down = dot(act_ref[...], wd_ref[...]).astype(BF)
    h = (wide + down.astype(F32)).astype(BF)
    h_ref[...] = h
    wide = h.astype(F32)
    b = wide * scale_of(wide)
    bt_ref[...] = b.T.astype(BF)
    b_ref[...] = b.astype(BF)
    dyt_ref[...] = dy_ref[...].astype(F32).T.astype(BF)


def adamw(w, m, v, g):
    m = 0.9 * m + 0.1 * g
    v = 0.95 * v + 0.05 * g * g
    step = m * lax.rsqrt(v + 1e-8) + 0.1 * w
    return (w - 0.02 * step).astype(BF), m, v


def backward(
    n, b_ref, bt_ref, dyi_ref, dyti_ref, h_ref, a_ref, at_ref, wg_ref, wu_ref, wd_ref,
    mg_ref, mu_ref, md_ref, vg_ref, vu_ref, vd_ref,
    ng_ref, nu_ref, nd_ref, omg_ref, omu_ref, omd_ref, ovg_ref, ovu_ref, ovd_ref,
    act, actt, dy, dyt, wg, wu, wd, dgu, prod, own_g, got_g, own_d, got_d, slot_g, slot_d,
    wo_g, wo_d, m_g, v_g, m_d, v_d,
    load, opt_load, pair_send, pair_got, rs_send, rs_got, ag_send, ag_got, fw_send, fw_got, keep_w, keep_m, keep_v,
    dpair_send, dpair_got, drs_send, drs_got, dag_send, dag_got, dfw_send, dfw_got, dkeep_w, dkeep_m, dkeep_v, credit,
):
    chips = n // 2
    tokens, d = dy.shape
    ff = wg.shape[1]
    width = ff // STRIPS
    rows, drows = d // n, ff // n
    half = drows // 2
    layers = wg_ref.shape[0]
    blocks = tokens // BLOCK
    turns = STRIPS + 1
    last = layers * turns - 2

    me = lax.axis_index("dp")
    z, c = me // 2, me % 2
    near = (((z + 1) % chips) * 2 + c, ((z + chips - 1) % chips) * 2 + c)
    mate = z * 2 + (1 - c)

    barrier = pltpu.get_barrier_semaphore()
    for other in (*near, mate):
        pl.semaphore_signal(barrier, inc=1, device_id={"dp": other}, device_id_type=MESH)
    pl.semaphore_wait(barrier, 3)

    def fetch(src, dst, k):
        return pltpu.make_async_copy(src, dst, load.at[k])

    top = layers - 1

    def loads(layer, acts, actst):
        return (
            fetch(acts, act, 0), fetch(wg_ref.at[layer], wg, 1), fetch(wu_ref.at[layer], wu, 2),
            fetch(wd_ref.at[layer], wd, 3), fetch(actst, actt, 4),
        )

    first = (*loads(top, b_ref, bt_ref), fetch(dyi_ref, dy, 5), fetch(dyti_ref, dyt, 6))
    for k in (0, 1, 2, 5, 3, 4, 6):
        first[k].start()
    mine = pl.ds(pl.multiple_of(me * rows, 8), rows)
    dmine = pl.ds(pl.multiple_of(me * drows, 8), drows)
    params = [
        (wg_ref.at[:, mine], wo_g.at[0]), (wu_ref.at[:, mine], wo_g.at[1]), (wd_ref.at[:, dmine], wo_d),
        (mg_ref, m_g.at[0]), (mu_ref, m_g.at[1]), (md_ref, m_d),
        (vg_ref, v_g.at[0]), (vu_ref, v_g.at[1]), (vd_ref, v_d),
    ]
    params = [pltpu.make_async_copy(s, t, opt_load.at[k]) for k, (s, t) in enumerate(params)]
    for copy in params:
        copy.start()

    second = loads(0, a_ref, at_ref)
    states = fetch(h_ref, act, 0)

    def remote(src, dst, send, got, to):
        return pltpu.make_async_remote_copy(src, dst, send, got, device_id={"dp": to}, device_id_type=MESH)

    def tok(t):
        return pl.ds(pl.multiple_of(t * BLOCK, BLOCK), BLOCK)

    def strip_block(j, t):
        cols = pl.ds(pl.multiple_of(j * width, width), width)
        a = act[tok(t), :]
        gate = dot(a, wg[:, cols])
        up = dot(a, wu[:, cols])
        dact = dot(dy[tok(t), :], wd[cols, :], ((1,), (1,))).astype(BF).astype(F32)
        sig = jax.nn.sigmoid(gate)
        silu = gate * sig
        prod[tok(t), :] = (silu * up).astype(BF)
        dgu[0, tok(t), cols] = (dact * up * (sig + silu * (1.0 - sig))).astype(BF)
        dgu[1, tok(t), cols] = (dact * silu).astype(BF)

    pieces = width // 256

    def weight_rows(j, k, piece):
        cols = pl.ds(pl.multiple_of(j * width + piece * 256, 256), 256)
        out = pl.ds(pl.multiple_of(piece * 256, 256), 256)
        total = dot(actt[...], dgu[k, :, cols])
        for chip in range(chips):
            for core in range(2):
                at = (chip * 2 + core) * rows
                own_g[j, core, k, chip, :, out] = total[at : at + rows].astype(BF)

    def down_rows(r, j, piece):
        total = dot(dyt[...], prod[:, pl.ds(pl.multiple_of(piece * 256, 256), 256)])
        total = total.T.astype(BF)
        per = 256 // (2 * drows)
        for k in range(per):
            for core in range(2):
                at = (k * 2 + core) * drows
                own_d[r, core, (j * pieces + piece) * per + k] = total[at : at + drows]

    def state_block(t):
        by_gate = dot(dgu[0, tok(t), :], wg[...], ((1,), (1,))).astype(BF)
        by_up = dot(dgu[1, tok(t), :], wu[...], ((1,), (1,))).astype(BF)
        by_a = (by_gate.astype(F32) + by_up.astype(F32)).astype(BF).astype(F32)
        wide = act[tok(t), :].astype(F32)
        scale = scale_of(wide)
        lean = jnp.mean(by_a * wide, -1, keepdims=True)
        by_h = (by_a * scale - wide * (scale * scale * scale * lean)).astype(BF)
        total = dy[tok(t), :].astype(F32) + by_h.astype(F32)
        dy[tok(t), :] = total.astype(BF)
        dyt[:, tok(t)] = total.astype(BF).astype(F32).T.astype(BF)

    def strip_outs(layer, j):
        return pl.ds(pl.multiple_of(j * width, width), width), (ng_ref, nu_ref)

    def block_of(k, chip):
        return pl.ds(pl.multiple_of((chip * 2 + c) * rows, 8), rows)

    def dblock_of(k, chip):
        return pl.ds(pl.multiple_of((chip * 2 + c) * drows + k * half, 8), half)

    def wrap(v):
        return lax.rem(v + 2 * chips, chips)

    def hop(k, step):
        return wrap(z - 1 - step) if k == 0 else wrap(z + 1 + step)

    def ag_hop(k, step):
        return wrap(z - step) if k == 0 else wrap(z + step)

    def ring_step(o, layer, j, q):
        for k in range(2):
            b = hop(k, o)
            mate_part = got_g[j, k, b].astype(F32) + own_g[j, c, k, b].astype(F32)

            @pl.when(o == 0)
            def _():
                slot_g[q, k, chips - 1] = mate_part.astype(BF)
                remote(slot_g.at[q, k, chips - 1], slot_g.at[q, k, 0], rs_send.at[q, k], rs_got.at[q, k, 0], near[k]).start()

            @pl.when(o > 0)
            def _():
                here = slot_g.at[q, k, o - 1]
                pltpu.make_async_copy(here, here, rs_got.at[q, k, o - 1]).wait()
                here[...] = (here[...].astype(F32) + mate_part).astype(BF)
                remote(here, slot_g.at[q, k, o], rs_send.at[q, k], rs_got.at[q, k, o], near[k]).start()

    def dring_step(o, layer, r):
        for k in range(2):
            b = hop(k, o)
            part = pl.ds(k * half, half)
            mate_part = got_d[b, part].astype(F32) + own_d[r, c, b, part].astype(F32)

            @pl.when(o == 0)
            def _():
                slot_d[r, k, chips - 1] = mate_part.astype(BF)
                remote(slot_d.at[r, k, chips - 1], slot_d.at[r, k, 0], drs_send.at[r, k], drs_got.at[r, k, 0], near[k]).start()

            @pl.when(o > 0)
            def _():
                here = slot_d.at[r, k, o - 1]
                pltpu.make_async_copy(here, here, drs_got.at[r, k, o - 1]).wait()
                here[...] = (here[...].astype(F32) + mate_part).astype(BF)
                remote(here, slot_d.at[r, k, o], drs_send.at[r, k], drs_got.at[r, k, o], near[k]).start()

    def publish(src, dst, keep, send, got, fsend, fgot, to):
        pltpu.make_async_copy(src, dst, keep).start()
        remote(src, dst, send, got, to).start()
        remote(src, dst, fsend, fgot, mate).start()

    def own_step(layer, j, q):
        cols, outs = strip_outs(layer, j)
        for k in range(2):
            here = slot_g.at[q, k, chips - 2]
            pltpu.make_async_copy(here, here, rs_got.at[q, k, chips - 2]).wait()
            mate_part = got_g[j, k, z].astype(F32) + own_g[j, c, k, z].astype(F32)
            g = (here[...].astype(F32) + mate_part).astype(BF).astype(F32)
            w1, m1, v1 = adamw(wo_g[k, layer, :, cols].astype(F32), m_g[k, layer, :, cols], v_g[k, layer, :, cols], g)
            m_g[k, layer, :, cols], v_g[k, layer, :, cols], here[...] = m1, v1, w1
            pltpu.make_async_copy(m_g.at[k, layer, :, cols], (omg_ref, omu_ref)[k].at[layer, :, cols], keep_m.at[q, k]).start()
            pltpu.make_async_copy(v_g.at[k, layer, :, cols], (ovg_ref, ovu_ref)[k].at[layer, :, cols], keep_v.at[q, k]).start()
            publish(
                here, outs[k].at[layer, block_of(k, z), cols], keep_w.at[q, k],
                ag_send.at[q, k], ag_got.at[q, k, 0], fw_send.at[q, k], fw_got.at[q, k], near[k],
            )

    def down_own_step(layer, r):
        for k in range(2):
            part = pl.ds(k * half, half)
            here = slot_d.at[r, k, chips - 2]
            pltpu.make_async_copy(here, here, drs_got.at[r, k, chips - 2]).wait()
            mate_part = got_d[z, part].astype(F32) + own_d[r, c, z, part].astype(F32)
            g = (here[...].astype(F32) + mate_part).astype(BF).astype(F32)
            w1, m1, v1 = adamw(wo_d[layer, part].astype(F32), m_d[layer, part], v_d[layer, part], g)
            m_d[layer, part], v_d[layer, part], here[...] = m1, v1, w1
            pltpu.make_async_copy(m_d.at[layer, part], omd_ref.at[layer, part], dkeep_m.at[r, k]).start()
            pltpu.make_async_copy(v_d.at[layer, part], ovd_ref.at[layer, part], dkeep_v.at[r, k]).start()
            publish(
                here, nd_ref.at[layer, dblock_of(k, z)], dkeep_w.at[r, k],
                dag_send.at[r, k], dag_got.at[r, k, 0], dfw_send.at[r, k], dfw_got.at[r, k], near[k],
            )

    def gather_step(s, layer, j, q):
        cols, outs = strip_outs(layer, j)
        for k in range(2):
            here = outs[k].at[layer, block_of(k, ag_hop(k, s)), cols]
            pltpu.make_async_copy(here, here, ag_got.at[q, k, s - 1]).wait()

            @pl.when(s < chips - 1)
            def _():
                remote(here, here, ag_send.at[q, k], ag_got.at[q, k, s], near[k]).start()

            remote(here, here, fw_send.at[q, k], fw_got.at[q, k], mate).start()

    def down_gather_step(s, layer, r):
        for k in range(2):
            here = nd_ref.at[layer, dblock_of(k, ag_hop(k, s))]
            pltpu.make_async_copy(here, here, dag_got.at[r, k, s - 1]).wait()

            @pl.when(s < chips - 1)
            def _():
                remote(here, here, dag_send.at[r, k], dag_got.at[r, k, s], near[k]).start()

            remote(here, here, dfw_send.at[r, k], dfw_got.at[r, k], mate).start()

    steps = 2 * chips - 1
    lags = steps // POINTS

    def point(i, p):
        def lag_step(idx, carry):
            lag = lags - idx
            g = i - lag
            r, j = g // turns, g % turns
            o = (lag - 1) * POINTS + p
            layer, q = top - r, r * STRIPS + j

            @pl.when((g >= 0) & (g <= last) & (j < STRIPS))
            def _():
                @pl.when(o == 0)
                def _():
                    pltpu.make_async_copy(got_g.at[j], got_g.at[j], pair_got.at[q]).wait()

                @pl.when(o < chips - 1)
                def _():
                    ring_step(o, layer, j, q)

                @pl.when(o == chips - 1)
                def _():
                    @pl.when(g == 0)
                    def _():
                        for copy in params:
                            copy.wait()

                    own_step(layer, j, q)

                @pl.when(o > chips - 1)
                def _():
                    gather_step(o - (chips - 1), layer, j, q)

                @pl.when(j == STRIPS - 1)
                def _():
                    @pl.when(o == 0)
                    def _():
                        pltpu.make_async_copy(got_d, got_d, dpair_got.at[r]).wait()

                    @pl.when(o < chips - 1)
                    def _():
                        dring_step(o, layer, r)

                    @pl.when(o == chips - 1)
                    def _():
                        down_own_step(layer, r)

                    @pl.when(o > chips - 1)
                    def _():
                        down_gather_step(o - (chips - 1), layer, r)

                @pl.when((o == chips - 1) & (r < layers - 1))
                def _():
                    pl.semaphore_signal(credit, inc=1, device_id={"dp": mate}, device_id_type=MESH)

            return carry

        lax.fori_loop(0, lags, lag_step, 0)

    def pair_copy(j, q):
        return remote(own_g.at[j, 1 - c], got_g.at[j], pair_send.at[q], pair_got.at[q], mate)

    def dpair_copy(r):
        return remote(own_d.at[r, 1 - c], got_d, dpair_send.at[r], dpair_got.at[r], mate)

    cut = (0, blocks // 2, blocks)

    def segment(i, p):
        r, j = i // turns, i % turns
        q = r * STRIPS + j
        strip = (i <= last) & (j < STRIPS)

        @pl.when((i == 0) & (p == 0))
        def _():
            for k in (0, 1, 2, 3, 5):
                first[k].wait()

        @pl.when((i == turns) & (p == 0))
        def _():
            for k in range(4):
                second[k].wait()

        @pl.when(strip & (p < 2))
        def _():
            def one(t, carry):
                strip_block(j, t)
                return carry

            lax.fori_loop(p * (blocks // 2), (p + 1) * (blocks // 2), one, 0)

        @pl.when(strip & (p == 1))
        def _():
            @pl.when(i == STRIPS - 1)
            def _():
                states.start()

        @pl.when((i == 0) & (p == 1))
        def _():
            for k in (4, 6):
                first[k].wait()

        @pl.when((i == turns) & (p == 1))
        def _():
            second[4].wait()

        @pl.when(strip & (p == 1) & (r > 0))
        def _():
            pair_copy(j, q - STRIPS).wait_send()

            @pl.when(j == 0)
            def _():
                dpair_copy(r - 1).wait_send()

        @pl.when(strip & (p > 0))
        def _():
            def one(e, carry):
                weight_rows(j, e // pieces, e % pieces)
                return carry

            lax.fori_loop((p - 1) * pieces, p * pieces, one, 0)

        @pl.when(strip & (p == POINTS - 1))
        def _():
            def one(e, carry):
                down_rows(r, j, e)
                return carry

            lax.fori_loop(0, pieces, one, 0)

            @pl.when(r > 0)
            def _():
                pl.semaphore_wait(credit, 1)

            pair_copy(j, q).start()

            @pl.when(j == STRIPS - 1)
            def _():
                dpair_copy(r).start()

        @pl.when((i < last) & (j == STRIPS))
        def _():
            @pl.when(p == 0)
            def _():
                second[3].start()
                states.wait()

            def one(t, carry):
                state_block(t)
                return carry

            lax.fori_loop((p * blocks) // POINTS, ((p + 1) * blocks) // POINTS, one, 0)

            @pl.when(p == POINTS - 1)
            def _():
                for k in (0, 1, 2, 4):
                    second[k].start()

    def turn(i, carry):
        def part(p, carry):
            segment(i, p)
            point(i, p)
            return carry

        return lax.fori_loop(0, POINTS, part, carry)

    lax.fori_loop(0, last + 1 + lags, turn, 0)

    def all_of(ref, sem):
        pltpu.make_async_copy(ref, ref, sem).wait()

    def finish(q, carry):
        j = lax.rem(q, STRIPS)
        layer = top - q // STRIPS
        cols, outs = strip_outs(layer, j)

        @pl.when(q >= (layers - 1) * STRIPS)
        def _():
            pair_copy(j, q).wait_send()

        for k in range(2):
            all_of(slot_g.at[q, k, pl.ds(0, chips - 1)], rs_send.at[q, k])
            all_of(slot_g.at[q, k, pl.ds(0, chips - 1)], ag_send.at[q, k])
            all_of(slot_g.at[q, k], fw_send.at[q, k])
            all_of(slot_g.at[q, k], fw_got.at[q, k])
            all_of(slot_g.at[q, k, 0], keep_w.at[q, k])
            all_of(m_g.at[k, layer, :, cols], keep_m.at[q, k])
            all_of(v_g.at[k, layer, :, cols], keep_v.at[q, k])
        return carry

    lax.fori_loop(0, layers * STRIPS, finish, 0)
    for r in range(layers):
        layer = top - r
        if r == layers - 1:
            dpair_copy(r).wait_send()
        for k in range(2):
            part = pl.ds(k * half, half)
            all_of(slot_d.at[r, k, pl.ds(0, chips - 1)], drs_send.at[r, k])
            all_of(slot_d.at[r, k, pl.ds(0, chips - 1)], dag_send.at[r, k])
            all_of(slot_d.at[r, k], dfw_send.at[r, k])
            all_of(slot_d.at[r, k], dfw_got.at[r, k])
            all_of(slot_d.at[r, k, 0], dkeep_w.at[r, k])
            all_of(m_d.at[layer, part], dkeep_m.at[r, k])
            all_of(v_d.at[layer, part], dkeep_v.at[r, k])


def solution(mesh):
    n = mesh.shape["dp"]

    def body(x, dy, wg, wu, wd, mg, mu, md, vg, vu, vd):
        x, dy = x[0], dy[0]
        tokens, d = x.shape
        layers, _, ff = wg.shape
        chips, rows, drows = n // 2, d // n, ff // n
        half, width = drows // 2, ff // STRIPS
        by_rows = pl.BlockSpec((BLOCK, d), lambda t: (t, 0))
        by_cols = pl.BlockSpec((d, BLOCK), lambda t: (0, t))
        tall, flat = jax.ShapeDtypeStruct((tokens, d), BF), jax.ShapeDtypeStruct((d, tokens), BF)
        up_spec = pl.BlockSpec((None, d, ff), lambda t: (0, 0, 0))
        down_spec = pl.BlockSpec((None, ff, d), lambda t: (0, 0, 0))
        a, at, h, b, bt, dyt = pl.pallas_call(
            forward,
            grid=(tokens // BLOCK,),
            in_specs=[by_rows, by_rows, up_spec, up_spec, down_spec],
            out_specs=[by_rows, by_cols, by_rows, by_rows, by_cols, by_cols],
            out_shape=[tall, flat, tall, tall, flat, flat],
            scratch_shapes=[pltpu.VMEM((BLOCK, ff), BF)],
            compiler_params=pltpu.CompilerParams(vmem_limit_bytes=60 * 2**20),
            name="forward",
        )(x, dy, wg, wu, wd)

        sds = jax.ShapeDtypeStruct
        vm, sem = pltpu.VMEM, pltpu.SemaphoreType.DMA
        q, r = layers * STRIPS, layers
        scratch = [
            vm((tokens, d), BF), vm((d, tokens), BF), vm((tokens, d), BF), vm((d, tokens), BF),
            vm((d, ff), BF), vm((d, ff), BF), vm((ff, d), BF),
            vm((2, tokens, ff), BF), vm((tokens, width), BF),
            vm((STRIPS, 2, 2, chips, rows, width), BF), vm((STRIPS, 2, chips, rows, width), BF),
            vm((layers, 2, chips, drows, d), BF), vm((chips, drows, d), BF),
            vm((q, 2, chips, rows, width), BF), vm((r, 2, chips, half, d), BF),
            vm((2, layers, rows, ff), BF), vm((layers, drows, d), BF),
            vm((2, layers, rows, ff), F32), vm((2, layers, rows, ff), F32),
            vm((layers, drows, d), F32), vm((layers, drows, d), F32),
            sem((7,)), sem((9,)), sem((q,)), sem((q,)),
            sem((q, 2)), sem((q, 2, chips - 1)), sem((q, 2)), sem((q, 2, chips - 1)), sem((q, 2)), sem((q, 2)),
            sem((q, 2)), sem((q, 2)), sem((q, 2)),
            sem((r,)), sem((r,)),
            sem((r, 2)), sem((r, 2, chips - 1)), sem((r, 2)), sem((r, 2, chips - 1)), sem((r, 2)), sem((r, 2)),
            sem((r, 2)), sem((r, 2)), sem((r, 2)),
            pltpu.SemaphoreType.REGULAR,
        ]
        return pl.pallas_call(
            functools.partial(backward, n),
            in_specs=[ANY] * 16,
            out_specs=[ANY] * 9,
            out_shape=[sds(t.shape, BF) for t in (wg, wu, wd)] + [sds(t.shape, F32) for t in (mg, mu, md, vg, vu, vd)],
            scratch_shapes=scratch,
            compiler_params=pltpu.CompilerParams(
                collective_id=0, has_side_effects=True, vmem_limit_bytes=67_043_328
            ),
            name="backward",
        )(b, bt, dy, dyt, h, a, at, wg, wu, wd, mg, mu, md, vg, vu, vd)

    seq, whole, rows = P(("rep", "dp"), None, None), P(None, None, None), P(None, "dp", None)
    return jax.shard_map(
        body,
        mesh=mesh,
        in_specs=(seq, seq, whole, whole, whole) + (rows,) * 6,
        out_specs=(P("rep", None, None),) * 3 + (P("rep", "dp", None),) * 6,
        check_vma=False,
    )
```

```python
import functools

import jax
import jax.numpy as jnp
from jax import lax
from jax.experimental import pallas as pl
from jax.experimental.pallas import tpu as pltpu
from jax.sharding import PartitionSpec as P

MESH = pl.DeviceIdType.MESH
BF, F32 = jnp.bfloat16, jnp.float32
BLOCK = 256
STRIPS = 4
POINTS = 3
ANY = pl.BlockSpec(memory_space=pl.ANY)


def dot(a, b, dims=((1,), (0,))):
    return lax.dot_general(a, b, (dims, ((), ())), preferred_element_type=F32)


def scale_of(wide):
    return lax.rsqrt(jnp.mean(wide * wide, -1, keepdims=True) + 1e-6)


def forward(x_ref, dy_ref, wg_ref, wu_ref, wd_ref, a_ref, at_ref, h_ref, b_ref, bt_ref, dyt_ref, act_ref):
    wide = x_ref[...].astype(F32)
    a = wide * scale_of(wide)
    at_ref[...] = a.T.astype(BF)
    a = a.astype(BF)
    a_ref[...] = a
    width = wg_ref.shape[1] // STRIPS
    for j in range(STRIPS):
        cols = slice(j * width, (j + 1) * width)
        gate, up = dot(a, wg_ref[:, cols]), dot(a, wu_ref[:, cols])
        act_ref[:, cols] = (gate * jax.nn.sigmoid(gate) * up).astype(BF)
    down = dot(act_ref[...], wd_ref[...]).astype(BF)
    h = (wide + down.astype(F32)).astype(BF)
    h_ref[...] = h
    wide = h.astype(F32)
    b = wide * scale_of(wide)
    bt_ref[...] = b.T.astype(BF)
    b_ref[...] = b.astype(BF)
    dyt_ref[...] = dy_ref[...].astype(F32).T.astype(BF)


def adamw(w, m, v, g):
    m = 0.9 * m + 0.1 * g
    v = 0.95 * v + 0.05 * g * g
    step = m * lax.rsqrt(v + 1e-8) + 0.1 * w
    return (w - 0.02 * step).astype(BF), m, v


def backward(
    n, b_ref, bt_ref, dyi_ref, dyti_ref, h_ref, a_ref, at_ref, wg_ref, wu_ref, wd_ref,
    mg_ref, mu_ref, md_ref, vg_ref, vu_ref, vd_ref,
    ng_ref, nu_ref, nd_ref, omg_ref, omu_ref, omd_ref, ovg_ref, ovu_ref, ovd_ref,
    act, actt, dy, dyt, wg, wu, wd, dgu, prod, own_g, got_g, own_d, got_d, slot_g, slot_d,
    wo_g, wo_d, m_g, v_g, m_d, v_d,
    load, opt_load, pair_send, pair_got, rs_start, rs_send, rs_got, ag_send, ag_got, fw_send, fw_got, keep_w, keep_m, keep_v,
    dpair_send, dpair_got, drs_start, drs_send, drs_got, dag_send, dag_got, dfw_send, dfw_got, dkeep_w, dkeep_m, dkeep_v, credit,
):
    chips = n // 2
    tokens, d = dy.shape
    ff = wg.shape[1]
    width = ff // STRIPS
    rows, drows = d // n, ff // n
    half = drows // 2
    layers = wg_ref.shape[0]
    blocks = tokens // BLOCK
    turns = STRIPS + 1
    last = layers * turns - 2

    me = lax.axis_index("dp")
    z, c = me // 2, me % 2
    near = (((z + 1) % chips) * 2 + c, ((z + chips - 1) % chips) * 2 + c)
    mate = z * 2 + (1 - c)

    barrier = pltpu.get_barrier_semaphore()
    for other in (*near, mate):
        pl.semaphore_signal(barrier, inc=1, device_id={"dp": other}, device_id_type=MESH)
    pl.semaphore_wait(barrier, 3)

    def fetch(src, dst, k):
        return pltpu.make_async_copy(src, dst, load.at[k])

    top = layers - 1

    def loads(layer, acts, actst):
        return (
            fetch(acts, act, 0), fetch(wg_ref.at[layer], wg, 1), fetch(wu_ref.at[layer], wu, 2),
            fetch(wd_ref.at[layer], wd, 3), fetch(actst, actt, 4),
        )

    first = (*loads(top, b_ref, bt_ref), fetch(dyi_ref, dy, 5), fetch(dyti_ref, dyt, 6))
    for k in (0, 1, 2, 5, 3, 4, 6):
        first[k].start()
    mine = pl.ds(pl.multiple_of(me * rows, 8), rows)
    dmine = pl.ds(pl.multiple_of(me * drows, 8), drows)
    params = [
        (wg_ref.at[:, mine], wo_g.at[0]), (wu_ref.at[:, mine], wo_g.at[1]), (wd_ref.at[:, dmine], wo_d),
        (mg_ref, m_g.at[0]), (mu_ref, m_g.at[1]), (md_ref, m_d),
        (vg_ref, v_g.at[0]), (vu_ref, v_g.at[1]), (vd_ref, v_d),
    ]
    params = [pltpu.make_async_copy(s, t, opt_load.at[k]) for k, (s, t) in enumerate(params)]
    for copy in params:
        copy.start()

    second = loads(0, a_ref, at_ref)
    states = fetch(h_ref, act, 0)

    def remote(src, dst, send, got, to):
        return pltpu.make_async_remote_copy(src, dst, send, got, device_id={"dp": to}, device_id_type=MESH)

    def tok(t):
        return pl.ds(pl.multiple_of(t * BLOCK, BLOCK), BLOCK)

    def strip_block(j, t):
        cols = pl.ds(pl.multiple_of(j * width, width), width)
        a = act[tok(t), :]
        gate = dot(a, wg[:, cols])
        up = dot(a, wu[:, cols])
        dact = dot(dy[tok(t), :], wd[cols, :], ((1,), (1,))).astype(BF).astype(F32)
        sig = jax.nn.sigmoid(gate)
        silu = gate * sig
        prod[tok(t), :] = (silu * up).astype(BF)
        dgu[0, tok(t), cols] = (dact * up * (sig + silu * (1.0 - sig))).astype(BF)
        dgu[1, tok(t), cols] = (dact * silu).astype(BF)

    pieces = width // 256

    def weight_rows(j, k, piece):
        cols = pl.ds(pl.multiple_of(j * width + piece * 256, 256), 256)
        out = pl.ds(pl.multiple_of(piece * 256, 256), 256)
        total = dot(actt[...], dgu[k, :, cols])
        for chip in range(chips):
            for core in range(2):
                at = (chip * 2 + core) * rows
                own_g[j, core, k, chip, :, out] = total[at : at + rows].astype(BF)

    def down_rows(r, j, piece):
        total = dot(dyt[...], prod[:, pl.ds(pl.multiple_of(piece * 256, 256), 256)])
        total = total.T.astype(BF)
        per = 256 // (2 * drows)
        for k in range(per):
            for core in range(2):
                at = (k * 2 + core) * drows
                own_d[r, core, (j * pieces + piece) * per + k] = total[at : at + drows]

    def state_block(t):
        by_gate = dot(dgu[0, tok(t), :], wg[...], ((1,), (1,))).astype(BF)
        by_up = dot(dgu[1, tok(t), :], wu[...], ((1,), (1,))).astype(BF)
        by_a = (by_gate.astype(F32) + by_up.astype(F32)).astype(BF).astype(F32)
        wide = act[tok(t), :].astype(F32)
        scale = scale_of(wide)
        lean = jnp.mean(by_a * wide, -1, keepdims=True)
        by_h = (by_a * scale - wide * (scale * scale * scale * lean)).astype(BF)
        total = dy[tok(t), :].astype(F32) + by_h.astype(F32)
        dy[tok(t), :] = total.astype(BF)
        dyt[:, tok(t)] = total.astype(BF).astype(F32).T.astype(BF)

    def strip_outs(layer, j):
        return pl.ds(pl.multiple_of(j * width, width), width), (ng_ref, nu_ref)

    def block_of(k, chip):
        return pl.ds(pl.multiple_of((chip * 2 + c) * rows, 8), rows)

    def dblock_of(k, chip):
        return pl.ds(pl.multiple_of((chip * 2 + c) * drows + k * half, 8), half)

    def wrap(v):
        return lax.rem(v + 2 * chips, chips)

    far = chips // 2
    ways = [((0, far - k, 0), (1, chips - 1 - (far - k), far - k)) for k in range(2)]

    def coming(way, length, o):
        return wrap(z + length - o) if way == 0 else wrap(z - length + o)

    def going(way, s):
        return wrap(z - s) if way == 0 else wrap(z + s)

    def ring_step(o, layer, j, q):
        for k in range(2):
            for way, length, base in ways[k]:

                @pl.when(o < length)
                def _():
                    b = coming(way, length, o)
                    own = own_g.at[j, c, k, b]
                    part = got_g[j, k, b].astype(F32) + own[...].astype(F32)

                    @pl.when(o == 0)
                    def _():
                        own[...] = part.astype(BF)
                        remote(own, slot_g.at[q, k, base], rs_start.at[q, k], rs_got.at[q, k, base], near[way]).start()

                    @pl.when(o > 0)
                    def _():
                        here = slot_g.at[q, k, base + o - 1]
                        pltpu.make_async_copy(here, here, rs_got.at[q, k, base + o - 1]).wait()
                        here[...] = (here[...].astype(F32) + part).astype(BF)
                        remote(here, slot_g.at[q, k, base + o], rs_send.at[q, k], rs_got.at[q, k, base + o], near[way]).start()

    def dring_step(o, layer, r):
        for k in range(2):
            rows_k = pl.ds(k * half, half)
            for way, length, base in ways[k]:

                @pl.when(o < length)
                def _():
                    b = coming(way, length, o)
                    own = own_d.at[r, c, b, rows_k]
                    part = got_d[b, rows_k].astype(F32) + own[...].astype(F32)

                    @pl.when(o == 0)
                    def _():
                        own[...] = part.astype(BF)
                        remote(own, slot_d.at[r, k, base], drs_start.at[r, k], drs_got.at[r, k, base], near[way]).start()

                    @pl.when(o > 0)
                    def _():
                        here = slot_d.at[r, k, base + o - 1]
                        pltpu.make_async_copy(here, here, drs_got.at[r, k, base + o - 1]).wait()
                        here[...] = (here[...].astype(F32) + part).astype(BF)
                        remote(here, slot_d.at[r, k, base + o], drs_send.at[r, k], drs_got.at[r, k, base + o], near[way]).start()

    def publish(src, dst, keep, send, got, fsend, fgot, k):
        pltpu.make_async_copy(src, dst, keep).start()
        for way, _, base in ways[k]:
            remote(src, dst, send, got.at[base], near[way]).start()
        remote(src, dst, fsend, fgot, mate).start()

    def arrived(slots, sems, starts, starting, k):
        pltpu.make_async_copy(starting, starting, starts).wait()
        first, second = (slots.at[base + length - 1] for _, length, base in ways[k])
        for (_, length, base), here in zip(ways[k], (first, second)):
            pltpu.make_async_copy(here, here, sems.at[base + length - 1]).wait()
        return first, first[...].astype(F32) + second[...].astype(F32)

    def own_step(layer, j, q):
        cols, outs = strip_outs(layer, j)
        for k in range(2):
            here, sums = arrived(slot_g.at[q, k], rs_got.at[q, k], rs_start.at[q, k], own_g.at[j, c, k, pl.ds(0, 2)], k)
            part = got_g[j, k, z].astype(F32) + own_g[j, c, k, z].astype(F32)
            g = (sums + part).astype(BF).astype(F32)
            w1, m1, v1 = adamw(wo_g[k, layer, :, cols].astype(F32), m_g[k, layer, :, cols], v_g[k, layer, :, cols], g)
            m_g[k, layer, :, cols], v_g[k, layer, :, cols], here[...] = m1, v1, w1
            publish(
                here, outs[k].at[layer, block_of(k, z), cols], keep_w.at[q, k],
                ag_send.at[q, k], ag_got.at[q, k], fw_send.at[q, k], fw_got.at[q, k], k,
            )
            pltpu.make_async_copy(m_g.at[k, layer, :, cols], (omg_ref, omu_ref)[k].at[layer, :, cols], keep_m.at[q, k]).start()
            pltpu.make_async_copy(v_g.at[k, layer, :, cols], (ovg_ref, ovu_ref)[k].at[layer, :, cols], keep_v.at[q, k]).start()

    def down_own_step(layer, r):
        for k in range(2):
            rows_k = pl.ds(k * half, half)
            starting = own_d.at[r, c, pl.ds(0, 2), rows_k]
            here, sums = arrived(slot_d.at[r, k], drs_got.at[r, k], drs_start.at[r, k], starting, k)
            part = got_d[z, rows_k].astype(F32) + own_d[r, c, z, rows_k].astype(F32)
            g = (sums + part).astype(BF).astype(F32)
            w1, m1, v1 = adamw(wo_d[layer, rows_k].astype(F32), m_d[layer, rows_k], v_d[layer, rows_k], g)
            m_d[layer, rows_k], v_d[layer, rows_k], here[...] = m1, v1, w1
            publish(
                here, nd_ref.at[layer, dblock_of(k, z)], dkeep_w.at[r, k],
                dag_send.at[r, k], dag_got.at[r, k], dfw_send.at[r, k], dfw_got.at[r, k], k,
            )
            pltpu.make_async_copy(m_d.at[layer, rows_k], omd_ref.at[layer, rows_k], dkeep_m.at[r, k]).start()
            pltpu.make_async_copy(v_d.at[layer, rows_k], ovd_ref.at[layer, rows_k], dkeep_v.at[r, k]).start()

    def hand_on(s, here_of, send, got, fsend, fgot, k):
        for way, length, base in ways[k]:

            @pl.when(s <= length)
            def _():
                here = here_of(going(way, s))
                pltpu.make_async_copy(here, here, got.at[base + s - 1]).wait()

                @pl.when(s < length)
                def _():
                    remote(here, here, send, got.at[base + s], near[way]).start()

                remote(here, here, fsend, fgot, mate).start()

    def gather_step(s, layer, j, q):
        cols, outs = strip_outs(layer, j)
        for k in range(2):
            hand_on(
                s, lambda b: outs[k].at[layer, block_of(k, b), cols],
                ag_send.at[q, k], ag_got.at[q, k], fw_send.at[q, k], fw_got.at[q, k], k,
            )

    def down_gather_step(s, layer, r):
        for k in range(2):
            hand_on(
                s, lambda b: nd_ref.at[layer, dblock_of(k, b)],
                dag_send.at[r, k], dag_got.at[r, k], dfw_send.at[r, k], dfw_got.at[r, k], k,
            )

    steps = 2 * far + 1
    lags = -(-steps // POINTS)

    def point(i, p):
        def lag_step(idx, carry):
            lag = lags - idx
            g = i - lag
            r, j = g // turns, g % turns
            o = (lag - 1) * POINTS + p
            layer, q = top - r, r * STRIPS + j

            @pl.when((g >= 0) & (g <= last) & (j < STRIPS))
            def _():
                @pl.when(o == 0)
                def _():
                    pltpu.make_async_copy(got_g.at[j], got_g.at[j], pair_got.at[q]).wait()

                @pl.when(o < far)
                def _():
                    ring_step(o, layer, j, q)

                @pl.when(o == far)
                def _():
                    @pl.when(g == 0)
                    def _():
                        for copy in params:
                            copy.wait()

                    own_step(layer, j, q)

                @pl.when(o > far)
                def _():
                    gather_step(o - far, layer, j, q)

                @pl.when(j == STRIPS - 1)
                def _():
                    @pl.when(o == 0)
                    def _():
                        pltpu.make_async_copy(got_d, got_d, dpair_got.at[r]).wait()

                    @pl.when(o < far)
                    def _():
                        dring_step(o, layer, r)

                    @pl.when(o == far)
                    def _():
                        down_own_step(layer, r)

                    @pl.when(o > far)
                    def _():
                        down_gather_step(o - far, layer, r)

                @pl.when((o == far) & (r < layers - 1))
                def _():
                    pl.semaphore_signal(credit, inc=1, device_id={"dp": mate}, device_id_type=MESH)

            return carry

        lax.fori_loop(0, lags, lag_step, 0)

    def pair_copy(j, q):
        return remote(own_g.at[j, 1 - c], got_g.at[j], pair_send.at[q], pair_got.at[q], mate)

    def dpair_copy(r):
        return remote(own_d.at[r, 1 - c], got_d, dpair_send.at[r], dpair_got.at[r], mate)

    cut = (0, blocks // 2, blocks)

    def segment(i, p):
        r, j = i // turns, i % turns
        q = r * STRIPS + j
        strip = (i <= last) & (j < STRIPS)

        @pl.when((i == 0) & (p == 0))
        def _():
            for k in (0, 1, 2, 3, 5):
                first[k].wait()

        @pl.when((i == turns) & (p == 0))
        def _():
            for k in range(4):
                second[k].wait()

        @pl.when(strip & (p < 2))
        def _():
            def one(t, carry):
                strip_block(j, t)
                return carry

            lax.fori_loop(p * (blocks // 2), (p + 1) * (blocks // 2), one, 0)

        @pl.when(strip & (p == 1))
        def _():
            @pl.when(i == STRIPS - 1)
            def _():
                states.start()

        @pl.when((i == 0) & (p == 1))
        def _():
            for k in (4, 6):
                first[k].wait()

        @pl.when((i == turns) & (p == 1))
        def _():
            second[4].wait()

        @pl.when(strip & (p == 1) & (r > 0))
        def _():
            pair_copy(j, q - STRIPS).wait_send()

            @pl.when(j == 0)
            def _():
                dpair_copy(r - 1).wait_send()

        @pl.when(strip & (p > 0))
        def _():
            def one(e, carry):
                weight_rows(j, e // pieces, e % pieces)
                return carry

            lax.fori_loop((p - 1) * pieces, p * pieces, one, 0)

        @pl.when(strip & (p == POINTS - 1))
        def _():
            def one(e, carry):
                down_rows(r, j, e)
                return carry

            lax.fori_loop(0, pieces, one, 0)

            @pl.when(r > 0)
            def _():
                pl.semaphore_wait(credit, 1)

            pair_copy(j, q).start()

            @pl.when(j == STRIPS - 1)
            def _():
                dpair_copy(r).start()

        @pl.when((i < last) & (j == STRIPS))
        def _():
            @pl.when(p == 0)
            def _():
                second[3].start()
                states.wait()

            def one(t, carry):
                state_block(t)
                return carry

            lax.fori_loop((p * blocks) // POINTS, ((p + 1) * blocks) // POINTS, one, 0)

            @pl.when(p == POINTS - 1)
            def _():
                for k in (0, 1, 2, 4):
                    second[k].start()

    def turn(i, carry):
        def part(p, carry):
            segment(i, p)
            point(i, p)
            return carry

        return lax.fori_loop(0, POINTS, part, carry)

    lax.fori_loop(0, last + 1 + lags, turn, 0)

    def all_of(ref, sem):
        pltpu.make_async_copy(ref, ref, sem).wait()

    def finish(q, carry):
        j = lax.rem(q, STRIPS)
        layer = top - q // STRIPS
        cols, outs = strip_outs(layer, j)

        @pl.when(q >= (layers - 1) * STRIPS)
        def _():
            pair_copy(j, q).wait_send()

        for k in range(2):
            all_of(slot_g.at[q, k, pl.ds(0, chips - 3)], rs_send.at[q, k])
            all_of(slot_g.at[q, k, pl.ds(0, chips - 1)], ag_send.at[q, k])
            all_of(got_g.at[j, k], fw_send.at[q, k])
            all_of(got_g.at[j, k], fw_got.at[q, k])
            all_of(slot_g.at[q, k, 0], keep_w.at[q, k])
            all_of(m_g.at[k, layer, :, cols], keep_m.at[q, k])
            all_of(v_g.at[k, layer, :, cols], keep_v.at[q, k])
        return carry

    lax.fori_loop(0, layers * STRIPS, finish, 0)
    for r in range(layers):
        layer = top - r
        if r == layers - 1:
            dpair_copy(r).wait_send()
        for k in range(2):
            part = pl.ds(k * half, half)
            all_of(slot_d.at[r, k, pl.ds(0, chips - 3)], drs_send.at[r, k])
            all_of(slot_d.at[r, k, pl.ds(0, chips - 1)], dag_send.at[r, k])
            all_of(got_d.at[:, part], dfw_send.at[r, k])
            all_of(got_d.at[:, part], dfw_got.at[r, k])
            all_of(slot_d.at[r, k, 0], dkeep_w.at[r, k])
            all_of(m_d.at[layer, part], dkeep_m.at[r, k])
            all_of(v_d.at[layer, part], dkeep_v.at[r, k])


def solution(mesh):
    n = mesh.shape["dp"]

    def body(x, dy, wg, wu, wd, mg, mu, md, vg, vu, vd):
        x, dy = x[0], dy[0]
        tokens, d = x.shape
        layers, _, ff = wg.shape
        chips, rows, drows = n // 2, d // n, ff // n
        half, width = drows // 2, ff // STRIPS
        by_rows = pl.BlockSpec((BLOCK, d), lambda t: (t, 0))
        by_cols = pl.BlockSpec((d, BLOCK), lambda t: (0, t))
        tall, flat = jax.ShapeDtypeStruct((tokens, d), BF), jax.ShapeDtypeStruct((d, tokens), BF)
        up_spec = pl.BlockSpec((None, d, ff), lambda t: (0, 0, 0))
        down_spec = pl.BlockSpec((None, ff, d), lambda t: (0, 0, 0))
        a, at, h, b, bt, dyt = pl.pallas_call(
            forward,
            grid=(tokens // BLOCK,),
            in_specs=[by_rows, by_rows, up_spec, up_spec, down_spec],
            out_specs=[by_rows, by_cols, by_rows, by_rows, by_cols, by_cols],
            out_shape=[tall, flat, tall, tall, flat, flat],
            scratch_shapes=[pltpu.VMEM((BLOCK, ff), BF)],
            compiler_params=pltpu.CompilerParams(vmem_limit_bytes=60 * 2**20),
            name="forward",
        )(x, dy, wg, wu, wd)

        sds = jax.ShapeDtypeStruct
        vm, sem = pltpu.VMEM, pltpu.SemaphoreType.DMA
        q, r = layers * STRIPS, layers
        scratch = [
            vm((tokens, d), BF), vm((d, tokens), BF), vm((tokens, d), BF), vm((d, tokens), BF),
            vm((d, ff), BF), vm((d, ff), BF), vm((ff, d), BF),
            vm((2, tokens, ff), BF), vm((tokens, width), BF),
            vm((STRIPS, 2, 2, chips, rows, width), BF), vm((STRIPS, 2, chips, rows, width), BF),
            vm((layers, 2, chips, drows, d), BF), vm((chips, drows, d), BF),
            vm((q, 2, chips - 1, rows, width), BF), vm((r, 2, chips - 1, half, d), BF),
            vm((2, layers, rows, ff), BF), vm((layers, drows, d), BF),
            vm((2, layers, rows, ff), F32), vm((2, layers, rows, ff), F32),
            vm((layers, drows, d), F32), vm((layers, drows, d), F32),
            sem((7,)), sem((9,)), sem((q,)), sem((q,)),
            sem((q, 2)), sem((q, 2)), sem((q, 2, chips - 1)), sem((q, 2)), sem((q, 2, chips - 1)), sem((q, 2)), sem((q, 2)),
            sem((q, 2)), sem((q, 2)), sem((q, 2)),
            sem((r,)), sem((r,)),
            sem((r, 2)), sem((r, 2)), sem((r, 2, chips - 1)), sem((r, 2)), sem((r, 2, chips - 1)), sem((r, 2)), sem((r, 2)),
            sem((r, 2)), sem((r, 2)), sem((r, 2)),
            pltpu.SemaphoreType.REGULAR,
        ]
        return pl.pallas_call(
            functools.partial(backward, n),
            in_specs=[ANY] * 16,
            out_specs=[ANY] * 9,
            out_shape=[sds(t.shape, BF) for t in (wg, wu, wd)] + [sds(t.shape, F32) for t in (mg, mu, md, vg, vu, vd)],
            scratch_shapes=scratch,
            compiler_params=pltpu.CompilerParams(
                collective_id=0, has_side_effects=True, vmem_limit_bytes=67_043_328
            ),
            name="backward",
        )(b, bt, dy, dyt, h, a, at, wg, wu, wd, mg, mu, md, vg, vu, vd)

    seq, whole, rows = P(("rep", "dp"), None, None), P(None, None, None), P(None, "dp", None)
    return jax.shard_map(
        body,
        mesh=mesh,
        in_specs=(seq, seq, whole, whole, whole) + (rows,) * 6,
        out_specs=(P("rep", None, None),) * 3 + (P("rep", "dp", None),) * 6,
        check_vma=False,
    )
```

```python
import functools

import jax
import jax.numpy as jnp
from jax import lax
from jax.experimental import pallas as pl
from jax.experimental.pallas import tpu as pltpu
from jax.sharding import PartitionSpec as P

MESH = pl.DeviceIdType.MESH
BF, F32 = jnp.bfloat16, jnp.float32
BLOCK = 512
TALL = 1024
STRIPS = 4
POINTS = 6
ANY = pl.BlockSpec(memory_space=pl.ANY)


def dot(a, b, dims=((1,), (0,))):
    return lax.dot_general(a, b, (dims, ((), ())), preferred_element_type=F32)


def scale_of(wide):
    return lax.rsqrt(jnp.mean(wide * wide, -1, keepdims=True) + 1e-6)


def forward(x_ref, dy_ref, wg_ref, wu_ref, wd_ref, a_ref, at_ref, h_ref, b_ref, bt_ref, dyt_ref, act_ref):
    wide = x_ref[...].astype(F32)
    a = wide * scale_of(wide)
    at_ref[...] = a.T.astype(BF)
    a = a.astype(BF)
    a_ref[...] = a
    width = wg_ref.shape[1] // STRIPS
    for j in range(STRIPS):
        cols = slice(j * width, (j + 1) * width)
        gate, up = dot(a, wg_ref[:, cols]), dot(a, wu_ref[:, cols])
        act_ref[:, cols] = (gate * jax.nn.sigmoid(gate) * up).astype(BF)
    down = dot(act_ref[...], wd_ref[...]).astype(BF)
    h = (wide + down.astype(F32)).astype(BF)
    h_ref[...] = h
    wide = h.astype(F32)
    b = wide * scale_of(wide)
    bt_ref[...] = b.T.astype(BF)
    b_ref[...] = b.astype(BF)
    dyt_ref[...] = dy_ref[...].astype(F32).T.astype(BF)


def adamw(w, m, v, g):
    m = 0.9 * m + 0.1 * g
    v = 0.95 * v + 0.05 * g * g
    step = m * lax.rsqrt(v + 1e-8) + 0.1 * w
    return (w - 0.02 * step).astype(BF), m, v


def backward(
    n, b_ref, bt_ref, dyi_ref, dyti_ref, h_ref, a_ref, at_ref, wg_ref, wu_ref, wd_ref,
    mg_ref, mu_ref, md_ref, vg_ref, vu_ref, vd_ref,
    ng_ref, nu_ref, nd_ref, omg_ref, omu_ref, omd_ref, ovg_ref, ovu_ref, ovd_ref,
    act, actt, dy, dyt, wg, wu, wd, dgu, prod, own_g, got_g, own_d, got_d, slot_g, slot_d,
    wo_g, wo_d, m_g, v_g, m_d, v_d,
    load, opt_load, pair_send, pair_got, rs_start, rs_send, rs_got, ag_send, ag_got, fw_send, fw_got, keep_w, keep_m, keep_v,
    dpair_send, dpair_got, drs_start, drs_send, drs_got, dag_send, dag_got, dfw_send, dfw_got, dkeep_w, dkeep_m, dkeep_v, credit,
):
    chips = n // 2
    tokens, d = dy.shape
    ff = wg.shape[1]
    width = ff // STRIPS
    rows, drows = d // n, ff // n
    half = drows // 2
    layers = wg_ref.shape[0]
    blocks = tokens // BLOCK
    turns = STRIPS + 1
    last = layers * turns - 2

    me = lax.axis_index("dp")
    z, c = me // 2, me % 2
    near = (((z + 1) % chips) * 2 + c, ((z + chips - 1) % chips) * 2 + c)
    mate = z * 2 + (1 - c)

    barrier = pltpu.get_barrier_semaphore()
    for other in (*near, mate):
        pl.semaphore_signal(barrier, inc=1, device_id={"dp": other}, device_id_type=MESH)
    pl.semaphore_wait(barrier, 3)

    def fetch(src, dst, k):
        return pltpu.make_async_copy(src, dst, load.at[k])

    top = layers - 1

    def loads(layer, acts, actst):
        return (
            fetch(acts, act, 0), fetch(wg_ref.at[layer], wg, 1), fetch(wu_ref.at[layer], wu, 2),
            fetch(wd_ref.at[layer], wd, 3), fetch(actst, actt, 4),
        )

    first = (*loads(top, b_ref, bt_ref), fetch(dyi_ref, dy, 5), fetch(dyti_ref, dyt, 6))
    for k in (0, 1, 2, 5, 3, 4, 6):
        first[k].start()
    mine = pl.ds(pl.multiple_of(me * rows, 8), rows)
    dmine = pl.ds(pl.multiple_of(me * drows, 8), drows)
    params = [
        (wg_ref.at[:, mine], wo_g.at[0]), (wu_ref.at[:, mine], wo_g.at[1]), (wd_ref.at[:, dmine], wo_d),
        (mg_ref, m_g.at[0]), (mu_ref, m_g.at[1]), (md_ref, m_d),
        (vg_ref, v_g.at[0]), (vu_ref, v_g.at[1]), (vd_ref, v_d),
    ]
    params = [pltpu.make_async_copy(s, t, opt_load.at[k]) for k, (s, t) in enumerate(params)]
    for copy in params:
        copy.start()

    second = loads(0, a_ref, at_ref)
    states = fetch(h_ref, act, 0)

    def remote(src, dst, send, got, to):
        return pltpu.make_async_remote_copy(src, dst, send, got, device_id={"dp": to}, device_id_type=MESH)

    def tok(t):
        return pl.ds(pl.multiple_of(t * BLOCK, BLOCK), BLOCK)

    pieces = width // 256
    slabs = tokens // TALL * pieces

    def strip_block(j, e):
        rows_e = pl.ds(pl.multiple_of(e // pieces * TALL, TALL), TALL)
        cols = pl.ds(pl.multiple_of(j * width + e % pieces * 256, 256), 256)
        here = pl.ds(pl.multiple_of(e % pieces * 256, 256), 256)
        a = act[rows_e, :]
        gate = dot(a, wg[:, cols])
        up = dot(a, wu[:, cols])
        dact = dot(dy[rows_e, :], wd[cols, :], ((1,), (1,))).astype(BF).astype(F32)
        sig = jax.nn.sigmoid(gate)
        silu = gate * sig
        prod[rows_e, here] = (silu * up).astype(BF)
        dgu[0, rows_e, cols] = (dact * up * (sig + silu * (1.0 - sig))).astype(BF)
        dgu[1, rows_e, cols] = (dact * silu).astype(BF)

    def weight_rows(q, j, k, piece):
        cols = pl.ds(pl.multiple_of(j * width + piece * 256, 256), 256)
        out = pl.ds(pl.multiple_of(piece * 256, 256), 256)
        total = dot(actt[...], dgu[k, :, cols])
        for chip in range(chips):
            for core in range(2):
                at = (chip * 2 + core) * rows
                own_g[jnp.where(c == core, j, STRIPS + q % 2), k, chip, :, out] = total[at : at + rows].astype(BF)

    def down_rows(r, j, piece):
        total = dot(dyt[...], prod[:, pl.ds(pl.multiple_of(piece * 256, 256), 256)])
        total = total.T.astype(BF)
        per = 256 // (2 * drows)
        for k in range(per):
            for core in range(2):
                at = (k * 2 + core) * drows
                own_d[jnp.where(c == core, r, layers), (j * pieces + piece) * per + k] = total[at : at + drows]

    def state_block(t):
        by_gate = dot(dgu[0, tok(t), :], wg[...], ((1,), (1,))).astype(BF)
        by_up = dot(dgu[1, tok(t), :], wu[...], ((1,), (1,))).astype(BF)
        by_a = (by_gate.astype(F32) + by_up.astype(F32)).astype(BF).astype(F32)
        wide = act[tok(t), :].astype(F32)
        scale = scale_of(wide)
        lean = jnp.mean(by_a * wide, -1, keepdims=True)
        by_h = (by_a * scale - wide * (scale * scale * scale * lean)).astype(BF)
        total = dy[tok(t), :].astype(F32) + by_h.astype(F32)
        dy[tok(t), :] = total.astype(BF)
        dyt[:, tok(t)] = total.astype(BF).astype(F32).T.astype(BF)

    def strip_outs(layer, j):
        return pl.ds(pl.multiple_of(j * width, width), width), (ng_ref, nu_ref)

    def block_of(k, chip):
        return pl.ds(pl.multiple_of((chip * 2 + c) * rows, 8), rows)

    def dblock_of(k, chip):
        return pl.ds(pl.multiple_of((chip * 2 + c) * drows + k * half, 8), half)

    def wrap(v):
        return lax.rem(v + 2 * chips, chips)

    far = chips // 2
    ways = [((0, far - k, 0), (1, chips - 1 - (far - k), far - k)) for k in range(2)]

    def coming(way, length, o):
        return wrap(z + length - o) if way == 0 else wrap(z - length + o)

    def going(way, s):
        return wrap(z - s) if way == 0 else wrap(z + s)

    def ring_step(o, layer, j, q, k):
        for way, length, base in ways[k]:

            @pl.when(o < length)
            def _():
                b = coming(way, length, o)
                own = own_g.at[j, k, b]
                part = got_g[j, k, b].astype(F32) + own[...].astype(F32)

                @pl.when(o == 0)
                def _():
                    own[...] = part.astype(BF)
                    remote(own, slot_g.at[q, k, base], rs_start.at[q, k], rs_got.at[q, k, base], near[way]).start()

                @pl.when(o > 0)
                def _():
                    here = slot_g.at[q, k, base + o - 1]
                    pltpu.make_async_copy(here, here, rs_got.at[q, k, base + o - 1]).wait()
                    here[...] = (here[...].astype(F32) + part).astype(BF)
                    remote(here, slot_g.at[q, k, base + o], rs_send.at[q, k], rs_got.at[q, k, base + o], near[way]).start()

    def dring_step(o, layer, r, k):
        rows_k = pl.ds(k * half, half)
        for way, length, base in ways[k]:

            @pl.when(o < length)
            def _():
                b = coming(way, length, o)
                own = own_d.at[r, b, rows_k]
                part = got_d[b, rows_k].astype(F32) + own[...].astype(F32)

                @pl.when(o == 0)
                def _():
                    own[...] = part.astype(BF)
                    remote(own, slot_d.at[r, k, base], drs_start.at[r, k], drs_got.at[r, k, base], near[way]).start()

                @pl.when(o > 0)
                def _():
                    here = slot_d.at[r, k, base + o - 1]
                    pltpu.make_async_copy(here, here, drs_got.at[r, k, base + o - 1]).wait()
                    here[...] = (here[...].astype(F32) + part).astype(BF)
                    remote(here, slot_d.at[r, k, base + o], drs_send.at[r, k], drs_got.at[r, k, base + o], near[way]).start()

    def publish(src, dst, keep, send, got, fsend, fgot, k):
        pltpu.make_async_copy(src, dst, keep).start()
        for way, _, base in ways[k]:
            remote(src, dst, send, got.at[base], near[way]).start()
        remote(src, dst, fsend, fgot, mate).start()

    def arrived(slots, sems, starts, starting, k):
        pltpu.make_async_copy(starting, starting, starts).wait()
        first, second = (slots.at[base + length - 1] for _, length, base in ways[k])
        for (_, length, base), here in zip(ways[k], (first, second)):
            pltpu.make_async_copy(here, here, sems.at[base + length - 1]).wait()
        return first, first[...].astype(F32) + second[...].astype(F32)

    def own_step(layer, j, q, k):
        cols, outs = strip_outs(layer, j)
        here, sums = arrived(slot_g.at[q, k], rs_got.at[q, k], rs_start.at[q, k], own_g.at[j, k, pl.ds(0, 2)], k)
        part = got_g[j, k, z].astype(F32) + own_g[j, k, z].astype(F32)
        g = (sums + part).astype(BF).astype(F32)
        w1, m1, v1 = adamw(wo_g[k, layer, :, cols].astype(F32), m_g[k, layer, :, cols], v_g[k, layer, :, cols], g)
        m_g[k, layer, :, cols], v_g[k, layer, :, cols], here[...] = m1, v1, w1
        publish(
            here, outs[k].at[layer, block_of(k, z), cols], keep_w.at[q, k],
            ag_send.at[q, k], ag_got.at[q, k], fw_send.at[q, k], fw_got.at[q, k], k,
        )
        pltpu.make_async_copy(m_g.at[k, layer, :, cols], (omg_ref, omu_ref)[k].at[layer, :, cols], keep_m.at[q, k]).start()
        pltpu.make_async_copy(v_g.at[k, layer, :, cols], (ovg_ref, ovu_ref)[k].at[layer, :, cols], keep_v.at[q, k]).start()

    def down_own_step(layer, r, k):
        rows_k = pl.ds(k * half, half)
        starting = own_d.at[r, pl.ds(0, 2), rows_k]
        here, sums = arrived(slot_d.at[r, k], drs_got.at[r, k], drs_start.at[r, k], starting, k)
        part = got_d[z, rows_k].astype(F32) + own_d[r, z, rows_k].astype(F32)
        g = (sums + part).astype(BF).astype(F32)
        w1, m1, v1 = adamw(wo_d[layer, rows_k].astype(F32), m_d[layer, rows_k], v_d[layer, rows_k], g)
        m_d[layer, rows_k], v_d[layer, rows_k], here[...] = m1, v1, w1
        publish(
            here, nd_ref.at[layer, dblock_of(k, z)], dkeep_w.at[r, k],
            dag_send.at[r, k], dag_got.at[r, k], dfw_send.at[r, k], dfw_got.at[r, k], k,
        )
        pltpu.make_async_copy(m_d.at[layer, rows_k], omd_ref.at[layer, rows_k], dkeep_m.at[r, k]).start()
        pltpu.make_async_copy(v_d.at[layer, rows_k], ovd_ref.at[layer, rows_k], dkeep_v.at[r, k]).start()

    def hand_on(s, here_of, send, got, fsend, fgot, k):
        for way, length, base in ways[k]:

            @pl.when(s <= length)
            def _():
                here = here_of(going(way, s))
                pltpu.make_async_copy(here, here, got.at[base + s - 1]).wait()

                @pl.when(s < length)
                def _():
                    remote(here, here, send, got.at[base + s], near[way]).start()

                remote(here, here, fsend, fgot, mate).start()

    def gather_step(s, layer, j, q, k):
        cols, outs = strip_outs(layer, j)
        hand_on(
            s, lambda b: outs[k].at[layer, block_of(k, b), cols],
            ag_send.at[q, k], ag_got.at[q, k], fw_send.at[q, k], fw_got.at[q, k], k,
        )

    def down_gather_step(s, layer, r, k):
        hand_on(
            s, lambda b: nd_ref.at[layer, dblock_of(k, b)],
            dag_send.at[r, k], dag_got.at[r, k], dfw_send.at[r, k], dfw_got.at[r, k], k,
        )

    steps = 2 * far + 1
    per = POINTS // 2
    lags = -(-steps // per)

    def point(i, p):
        def advance(lag, k):
            g = i - lag
            r, j = g // turns, g % turns
            o = (lag - 1) * per + p // 2
            layer, q = top - r, r * STRIPS + j

            @pl.when((g >= 0) & (g <= last) & (j < STRIPS))
            def _():
                if k == 0:

                    @pl.when(o == 0)
                    def _():
                        pltpu.make_async_copy(got_g.at[j], got_g.at[j], pair_got.at[q]).wait()

                    @pl.when((o == 0) & (j == STRIPS - 1))
                    def _():
                        pltpu.make_async_copy(got_d, got_d, dpair_got.at[r]).wait()

                    @pl.when((o == far) & (g == 0))
                    def _():
                        for copy in params:
                            copy.wait()

                @pl.when(o < far)
                def _():
                    ring_step(o, layer, j, q, k)

                @pl.when(o == far)
                def _():
                    own_step(layer, j, q, k)

                @pl.when(o > far)
                def _():
                    gather_step(o - far, layer, j, q, k)

                @pl.when(j == STRIPS - 1)
                def _():
                    @pl.when(o < far)
                    def _():
                        dring_step(o, layer, r, k)

                    @pl.when(o == far)
                    def _():
                        down_own_step(layer, r, k)

                    @pl.when(o > far)
                    def _():
                        down_gather_step(o - far, layer, r, k)

                if k == 1:

                    @pl.when((o == far) & (r < layers - 1))
                    def _():
                        pl.semaphore_signal(credit, inc=1, device_id={"dp": mate}, device_id_type=MESH)

        for k in range(2):

            @pl.when(p % 2 == k)
            def _():
                def lag_step(idx, carry):
                    advance(lags - idx, k)
                    return carry

                lax.fori_loop(0, lags, lag_step, 0)

    def pair_copy(j, q):
        return remote(own_g.at[STRIPS + q % 2], got_g.at[j], pair_send.at[q], pair_got.at[q], mate)

    def dpair_copy(r):
        return remote(own_d.at[layers], got_d, dpair_send.at[r], dpair_got.at[r], mate)

    def segment(i, p):
        r, j = i // turns, i % turns
        q = r * STRIPS + j
        strip = (i <= last) & (j < STRIPS)

        @pl.when((i == 0) & (p == 0))
        def _():
            for k in (0, 1, 2, 3, 5):
                first[k].wait()

        @pl.when((i == turns) & (p == 0))
        def _():
            for k in range(4):
                second[k].wait()

        @pl.when(strip & (p < slabs))
        def _():
            strip_block(j, p)

        @pl.when((i == STRIPS - 1) & (p == slabs))
        def _():
            states.start()

        @pl.when((i == 0) & (p == slabs - 1))
        def _():
            for k in (4, 6):
                first[k].wait()

        @pl.when((i == turns) & (p == slabs - 1))
        def _():
            second[4].wait()

        @pl.when(strip & (p == slabs - 1))
        def _():
            @pl.when(q >= 2)
            def _():
                pair_copy(j, q - 2).wait_send()

            @pl.when((r > 0) & (j == 0))
            def _():
                dpair_copy(r - 1).wait_send()

        @pl.when(strip & (p >= slabs - 1))
        def _():
            def one(e, carry):
                weight_rows(q, j, e // pieces, e % pieces)
                return carry

            ahead = p - (slabs - 1)
            lax.fori_loop(jnp.maximum(2 * ahead - 1, 0), jnp.minimum(2 * ahead + 1, 2 * pieces), one, 0)

        @pl.when(strip & (p == POINTS - 1))
        def _():
            def one(e, carry):
                down_rows(r, j, e)
                return carry

            lax.fori_loop(0, pieces, one, 0)

            @pl.when(r > 0)
            def _():
                pl.semaphore_wait(credit, 1)

            pair_copy(j, q).start()

            @pl.when(j == STRIPS - 1)
            def _():
                dpair_copy(r).start()

        @pl.when((i < last) & (j == STRIPS))
        def _():
            @pl.when(p == 0)
            def _():
                second[3].start()
                states.wait()

            def one(t, carry):
                state_block(t)
                return carry

            lax.fori_loop((p * blocks) // POINTS, ((p + 1) * blocks) // POINTS, one, 0)

            @pl.when(p == POINTS - 1)
            def _():
                for k in (0, 1, 2, 4):
                    second[k].start()

    def turn(i, carry):
        def part(p, carry):
            segment(i, p)
            point(i, p)
            return carry

        return lax.fori_loop(0, POINTS, part, carry)

    lax.fori_loop(0, last + 1 + lags, turn, 0)

    def all_of(ref, sem):
        pltpu.make_async_copy(ref, ref, sem).wait()

    def finish(q, carry):
        j = lax.rem(q, STRIPS)
        layer = top - q // STRIPS
        cols, outs = strip_outs(layer, j)

        @pl.when(q >= layers * STRIPS - 2)
        def _():
            pair_copy(j, q).wait_send()

        for k in range(2):
            all_of(slot_g.at[q, k, pl.ds(0, chips - 3)], rs_send.at[q, k])
            all_of(slot_g.at[q, k, pl.ds(0, chips - 1)], ag_send.at[q, k])
            all_of(got_g.at[j, k], fw_send.at[q, k])
            all_of(got_g.at[j, k], fw_got.at[q, k])
            all_of(slot_g.at[q, k, 0], keep_w.at[q, k])
            all_of(m_g.at[k, layer, :, cols], keep_m.at[q, k])
            all_of(v_g.at[k, layer, :, cols], keep_v.at[q, k])
        return carry

    lax.fori_loop(0, layers * STRIPS, finish, 0)
    for r in range(layers):
        layer = top - r
        if r == layers - 1:
            dpair_copy(r).wait_send()
        for k in range(2):
            part = pl.ds(k * half, half)
            all_of(slot_d.at[r, k, pl.ds(0, chips - 3)], drs_send.at[r, k])
            all_of(slot_d.at[r, k, pl.ds(0, chips - 1)], dag_send.at[r, k])
            all_of(got_d.at[:, part], dfw_send.at[r, k])
            all_of(got_d.at[:, part], dfw_got.at[r, k])
            all_of(slot_d.at[r, k, 0], dkeep_w.at[r, k])
            all_of(m_d.at[layer, part], dkeep_m.at[r, k])
            all_of(v_d.at[layer, part], dkeep_v.at[r, k])


def solution(mesh):
    n = mesh.shape["dp"]

    def body(x, dy, wg, wu, wd, mg, mu, md, vg, vu, vd):
        x, dy = x[0], dy[0]
        tokens, d = x.shape
        layers, _, ff = wg.shape
        chips, rows, drows = n // 2, d // n, ff // n
        half, width = drows // 2, ff // STRIPS
        by_rows = pl.BlockSpec((BLOCK, d), lambda t: (t, 0))
        by_cols = pl.BlockSpec((d, BLOCK), lambda t: (0, t))
        tall, flat = jax.ShapeDtypeStruct((tokens, d), BF), jax.ShapeDtypeStruct((d, tokens), BF)
        up_spec = pl.BlockSpec((None, d, ff), lambda t: (0, 0, 0))
        down_spec = pl.BlockSpec((None, ff, d), lambda t: (0, 0, 0))
        a, at, h, b, bt, dyt = pl.pallas_call(
            forward,
            grid=(tokens // BLOCK,),
            in_specs=[by_rows, by_rows, up_spec, up_spec, down_spec],
            out_specs=[by_rows, by_cols, by_rows, by_rows, by_cols, by_cols],
            out_shape=[tall, flat, tall, tall, flat, flat],
            scratch_shapes=[pltpu.VMEM((BLOCK, ff), BF)],
            compiler_params=pltpu.CompilerParams(vmem_limit_bytes=60 * 2**20),
            name="forward",
        )(x, dy, wg, wu, wd)

        sds = jax.ShapeDtypeStruct
        vm, sem = pltpu.VMEM, pltpu.SemaphoreType.DMA
        q, r = layers * STRIPS, layers
        scratch = [
            vm((tokens, d), BF), vm((d, tokens), BF), vm((tokens, d), BF), vm((d, tokens), BF),
            vm((d, ff), BF), vm((d, ff), BF), vm((ff, d), BF),
            vm((2, tokens, ff), BF), vm((tokens, width), BF),
            vm((STRIPS + 2, 2, chips, rows, width), BF), vm((STRIPS, 2, chips, rows, width), BF),
            vm((layers + 1, chips, drows, d), BF), vm((chips, drows, d), BF),
            vm((q, 2, chips - 1, rows, width), BF), vm((r, 2, chips - 1, half, d), BF),
            vm((2, layers, rows, ff), BF), vm((layers, drows, d), BF),
            vm((2, layers, rows, ff), F32), vm((2, layers, rows, ff), F32),
            vm((layers, drows, d), F32), vm((layers, drows, d), F32),
            sem((7,)), sem((9,)), sem((q,)), sem((q,)),
            sem((q, 2)), sem((q, 2)), sem((q, 2, chips - 1)), sem((q, 2)), sem((q, 2, chips - 1)), sem((q, 2)), sem((q, 2)),
            sem((q, 2)), sem((q, 2)), sem((q, 2)),
            sem((r,)), sem((r,)),
            sem((r, 2)), sem((r, 2)), sem((r, 2, chips - 1)), sem((r, 2)), sem((r, 2, chips - 1)), sem((r, 2)), sem((r, 2)),
            sem((r, 2)), sem((r, 2)), sem((r, 2)),
            pltpu.SemaphoreType.REGULAR,
        ]
        return pl.pallas_call(
            functools.partial(backward, n),
            in_specs=[ANY] * 16,
            out_specs=[ANY] * 9,
            out_shape=[sds(t.shape, BF) for t in (wg, wu, wd)] + [sds(t.shape, F32) for t in (mg, mu, md, vg, vu, vd)],
            scratch_shapes=scratch,
            compiler_params=pltpu.CompilerParams(
                collective_id=0, has_side_effects=True, vmem_limit_bytes=67_043_328
            ),
            name="backward",
        )(b, bt, dy, dyt, h, a, at, wg, wu, wd, mg, mu, md, vg, vu, vd)

    seq, whole, rows = P(("rep", "dp"), None, None), P(None, None, None), P(None, "dp", None)
    return jax.shard_map(
        body,
        mesh=mesh,
        in_specs=(seq, seq, whole, whole, whole) + (rows,) * 6,
        out_specs=(P("rep", None, None),) * 3 + (P("rep", "dp", None),) * 6,
        check_vma=False,
    )
```

```python
import functools

import jax
import jax.numpy as jnp
from jax import lax
from jax.experimental import pallas as pl
from jax.experimental.pallas import tpu as pltpu
from jax.sharding import PartitionSpec as P

MESH = pl.DeviceIdType.MESH
BF, F32 = jnp.bfloat16, jnp.float32
BLOCK = 512
TALL = 1024
STRIPS = 4
POINTS = 6
ANY = pl.BlockSpec(memory_space=pl.ANY)


def dot(a, b, dims=((1,), (0,))):
    return lax.dot_general(a, b, (dims, ((), ())), preferred_element_type=F32)


def scale_of(wide):
    return lax.rsqrt(jnp.mean(wide * wide, -1, keepdims=True) + 1e-6)


def adamw(w, m, v, g):
    m = 0.9 * m + 0.1 * g
    v = 0.95 * v + 0.05 * g * g
    step = m * lax.rsqrt(v + 1e-8) + 0.1 * w
    return (w - 0.02 * step).astype(BF), m, v


def train(
    n, x_ref, dyi_ref, wg_ref, wu_ref, wd_ref,
    mg_ref, mu_ref, md_ref, vg_ref, vu_ref, vd_ref,
    ng_ref, nu_ref, nd_ref, omg_ref, omu_ref, omd_ref, ovg_ref, ovu_ref, ovd_ref, h_ref, a_ref, at_ref,
    act, actt, dy, dyt, wg, wu, wd, dgu, prod, own_g, got_g, own_d, got_d, slot_g, slot_d,
    wo_g, wo_d, m_g, v_g, m_d, v_d,
    load, x_load, first_out, opt_load, pair_send, pair_got, rs_start, rs_send, rs_got, ag_send, ag_got, fw_send, fw_got, keep_w, keep_m, keep_v,
    dpair_send, dpair_got, drs_start, drs_send, drs_got, dag_send, dag_got, dfw_send, dfw_got, dkeep_w, dkeep_m, dkeep_v, credit,
):
    chips = n // 2
    tokens, d = dy.shape
    ff = wg.shape[1]
    width = ff // STRIPS
    rows, drows = d // n, ff // n
    half = drows // 2
    layers = wg_ref.shape[0]
    blocks = tokens // BLOCK
    turns = STRIPS + 1
    last = layers * turns - 2

    me = lax.axis_index("dp")
    z, c = me // 2, me % 2
    near = (((z + 1) % chips) * 2 + c, ((z + chips - 1) % chips) * 2 + c)
    mate = z * 2 + (1 - c)

    barrier = pltpu.get_barrier_semaphore()
    for other in (*near, mate):
        pl.semaphore_signal(barrier, inc=1, device_id={"dp": other}, device_id_type=MESH)
    pl.semaphore_wait(barrier, 3)

    def fetch(src, dst, k):
        return pltpu.make_async_copy(src, dst, load.at[k])

    top = layers - 1

    def tok(t):
        return pl.ds(pl.multiple_of(t * BLOCK, BLOCK), BLOCK)

    def loads(layer, acts, actst):
        return (
            fetch(acts, act, 0), fetch(wg_ref.at[layer], wg, 1), fetch(wu_ref.at[layer], wu, 2),
            fetch(wd_ref.at[layer], wd, 3), fetch(actst, actt, 4),
        )

    wg_v, wu_v, at_v = (dgu.at[0, pl.ds(k * d, d)] for k in range(3))
    wd_v, x_v, h_v = (dgu.at[1, :, pl.ds(k * d, d)] for k in range(3))

    def x_copy(t):
        return pltpu.make_async_copy(x_ref.at[tok(t)], x_v.at[tok(t)], x_load.at[t])

    early = (fetch(wg_ref.at[0], wg_v, 5), fetch(wu_ref.at[0], wu_v, 6), fetch(wd_ref.at[0], wd_v, 7), fetch(dyi_ref, dy, 8))
    first = (None, fetch(wg_ref.at[top], wg, 1), fetch(wu_ref.at[top], wu, 2), fetch(wd_ref.at[top], wd, 3))
    x_copy(0).start()
    for copy in early:
        copy.start()
    for t in range(1, blocks):
        x_copy(t).start()
    for copy in first[1:]:
        copy.start()
    mine = pl.ds(pl.multiple_of(me * rows, 8), rows)
    dmine = pl.ds(pl.multiple_of(me * drows, 8), drows)
    params = [
        (wg_ref.at[:, mine], wo_g.at[0]), (wu_ref.at[:, mine], wo_g.at[1]), (wd_ref.at[:, dmine], wo_d),
        (mg_ref, m_g.at[0]), (mu_ref, m_g.at[1]), (md_ref, m_d),
        (vg_ref, v_g.at[0]), (vu_ref, v_g.at[1]), (vd_ref, v_d),
    ]
    params = [pltpu.make_async_copy(s, t, opt_load.at[k]) for k, (s, t) in enumerate(params)]
    for copy in params:
        copy.start()

    second = loads(0, a_ref, at_ref)
    states = fetch(h_ref, act, 0)

    def remote(src, dst, send, got, to):
        return pltpu.make_async_remote_copy(src, dst, send, got, device_id={"dp": to}, device_id_type=MESH)

    def first_outs(part):
        return (
            pltpu.make_async_copy(x_v.at[part], a_ref.at[part], first_out.at[0]),
            pltpu.make_async_copy(at_v.at[:, part], at_ref.at[:, part], first_out.at[1]),
            pltpu.make_async_copy(h_v.at[part], h_ref.at[part], first_out.at[2]),
        )

    def forward_block(t):
        x_copy(t).wait()
        part = tok(t)
        wide = x_v[part, :].astype(F32)
        a = wide * scale_of(wide)
        at_v[:, part] = a.T.astype(BF)
        a = a.astype(BF)
        for j in range(STRIPS):
            cols = slice(j * width, (j + 1) * width)
            gate, up = dot(a, wg_v[:, cols]), dot(a, wu_v[:, cols])
            prod[j * BLOCK : (j + 1) * BLOCK, :] = (gate * jax.nn.sigmoid(gate) * up).astype(BF)

        @pl.when(t == 0)
        def _():
            early[2].wait()
            early[3].wait()

        down = sum(
            dot(prod[j * BLOCK : (j + 1) * BLOCK, :], wd_v[j * width : (j + 1) * width, :]) for j in range(STRIPS)
        ).astype(BF)
        h = (wide + down.astype(F32)).astype(BF)
        x_v[part, :] = a
        h_v[part, :] = h
        wide = h.astype(F32)
        b = wide * scale_of(wide)
        actt[:, part] = b.T.astype(BF)
        act[part, :] = b.astype(BF)
        dyt[:, part] = dy[part, :].astype(F32).T.astype(BF)
        for copy in first_outs(part):
            copy.start()

    early[0].wait()
    early[1].wait()

    def forward_step(t, carry):
        forward_block(t)
        return carry

    lax.fori_loop(0, blocks, forward_step, 0)
    for copy in first_outs(pl.ds(0, tokens)):
        copy.wait()

    pieces = width // 256
    slabs = tokens // TALL * pieces

    def strip_block(j, e):
        rows_e = pl.ds(pl.multiple_of(e // pieces * TALL, TALL), TALL)
        cols = pl.ds(pl.multiple_of(j * width + e % pieces * 256, 256), 256)
        here = pl.ds(pl.multiple_of(e % pieces * 256, 256), 256)
        a = act[rows_e, :]
        gate = dot(a, wg[:, cols])
        up = dot(a, wu[:, cols])
        dact = dot(dy[rows_e, :], wd[cols, :], ((1,), (1,))).astype(BF).astype(F32)
        sig = jax.nn.sigmoid(gate)
        silu = gate * sig
        prod[rows_e, here] = (silu * up).astype(BF)
        dgu[0, rows_e, cols] = (dact * up * (sig + silu * (1.0 - sig))).astype(BF)
        dgu[1, rows_e, cols] = (dact * silu).astype(BF)

    def weight_rows(q, j, k, piece):
        cols = pl.ds(pl.multiple_of(j * width + piece * 256, 256), 256)
        out = pl.ds(pl.multiple_of(piece * 256, 256), 256)
        total = dot(actt[...], dgu[k, :, cols])
        for chip in range(chips):
            for core in range(2):
                at = (chip * 2 + core) * rows
                own_g[jnp.where(c == core, j, STRIPS + q % 2), k, chip, :, out] = total[at : at + rows].astype(BF)

    def down_rows(r, j, piece):
        total = dot(dyt[...], prod[:, pl.ds(pl.multiple_of(piece * 256, 256), 256)])
        total = total.T.astype(BF)
        per = 256 // (2 * drows)
        for k in range(per):
            for core in range(2):
                at = (k * 2 + core) * drows
                own_d[jnp.where(c == core, r, layers), (j * pieces + piece) * per + k] = total[at : at + drows]

    def state_block(t):
        by_gate = dot(dgu[0, tok(t), :], wg[...], ((1,), (1,))).astype(BF)
        by_up = dot(dgu[1, tok(t), :], wu[...], ((1,), (1,))).astype(BF)
        by_a = (by_gate.astype(F32) + by_up.astype(F32)).astype(BF).astype(F32)
        wide = act[tok(t), :].astype(F32)
        scale = scale_of(wide)
        lean = jnp.mean(by_a * wide, -1, keepdims=True)
        by_h = (by_a * scale - wide * (scale * scale * scale * lean)).astype(BF)
        total = dy[tok(t), :].astype(F32) + by_h.astype(F32)
        dy[tok(t), :] = total.astype(BF)
        dyt[:, tok(t)] = total.astype(BF).astype(F32).T.astype(BF)

    def strip_outs(layer, j):
        return pl.ds(pl.multiple_of(j * width, width), width), (ng_ref, nu_ref)

    def block_of(k, chip):
        return pl.ds(pl.multiple_of((chip * 2 + c) * rows, 8), rows)

    def dblock_of(k, chip):
        return pl.ds(pl.multiple_of((chip * 2 + c) * drows + k * half, 8), half)

    def wrap(v):
        return lax.rem(v + 2 * chips, chips)

    far = chips // 2
    ways = [((0, far - k, 0), (1, chips - 1 - (far - k), far - k)) for k in range(2)]

    def coming(way, length, o):
        return wrap(z + length - o) if way == 0 else wrap(z - length + o)

    def going(way, s):
        return wrap(z - s) if way == 0 else wrap(z + s)

    def ring_step(o, layer, j, q, k):
        for way, length, base in ways[k]:

            @pl.when(o < length)
            def _():
                b = coming(way, length, o)
                own = own_g.at[j, k, b]
                part = got_g[j, k, b].astype(F32) + own[...].astype(F32)

                @pl.when(o == 0)
                def _():
                    own[...] = part.astype(BF)
                    remote(own, slot_g.at[q, k, base], rs_start.at[q, k], rs_got.at[q, k, base], near[way]).start()

                @pl.when(o > 0)
                def _():
                    here = slot_g.at[q, k, base + o - 1]
                    pltpu.make_async_copy(here, here, rs_got.at[q, k, base + o - 1]).wait()
                    here[...] = (here[...].astype(F32) + part).astype(BF)
                    remote(here, slot_g.at[q, k, base + o], rs_send.at[q, k], rs_got.at[q, k, base + o], near[way]).start()

    def dring_step(o, layer, r, k):
        rows_k = pl.ds(k * half, half)
        for way, length, base in ways[k]:

            @pl.when(o < length)
            def _():
                b = coming(way, length, o)
                own = own_d.at[r, b, rows_k]
                part = got_d[b, rows_k].astype(F32) + own[...].astype(F32)

                @pl.when(o == 0)
                def _():
                    own[...] = part.astype(BF)
                    remote(own, slot_d.at[r, k, base], drs_start.at[r, k], drs_got.at[r, k, base], near[way]).start()

                @pl.when(o > 0)
                def _():
                    here = slot_d.at[r, k, base + o - 1]
                    pltpu.make_async_copy(here, here, drs_got.at[r, k, base + o - 1]).wait()
                    here[...] = (here[...].astype(F32) + part).astype(BF)
                    remote(here, slot_d.at[r, k, base + o], drs_send.at[r, k], drs_got.at[r, k, base + o], near[way]).start()

    def publish(src, dst, keep, send, got, fsend, fgot, k):
        pltpu.make_async_copy(src, dst, keep).start()
        for way, _, base in ways[k]:
            remote(src, dst, send, got.at[base], near[way]).start()
        remote(src, dst, fsend, fgot, mate).start()

    def arrived(slots, sems, starts, starting, k):
        pltpu.make_async_copy(starting, starting, starts).wait()
        first, second = (slots.at[base + length - 1] for _, length, base in ways[k])
        for (_, length, base), here in zip(ways[k], (first, second)):
            pltpu.make_async_copy(here, here, sems.at[base + length - 1]).wait()
        return first, first[...].astype(F32) + second[...].astype(F32)

    def own_step(layer, j, q, k):
        cols, outs = strip_outs(layer, j)
        here, sums = arrived(slot_g.at[q, k], rs_got.at[q, k], rs_start.at[q, k], own_g.at[j, k, pl.ds(0, 2)], k)
        part = got_g[j, k, z].astype(F32) + own_g[j, k, z].astype(F32)
        g = (sums + part).astype(BF).astype(F32)
        w1, m1, v1 = adamw(wo_g[k, layer, :, cols].astype(F32), m_g[k, layer, :, cols], v_g[k, layer, :, cols], g)
        m_g[k, layer, :, cols], v_g[k, layer, :, cols], here[...] = m1, v1, w1
        publish(
            here, outs[k].at[layer, block_of(k, z), cols], keep_w.at[q, k],
            ag_send.at[q, k], ag_got.at[q, k], fw_send.at[q, k], fw_got.at[q, k], k,
        )
        pltpu.make_async_copy(m_g.at[k, layer, :, cols], (omg_ref, omu_ref)[k].at[layer, :, cols], keep_m.at[q, k]).start()
        pltpu.make_async_copy(v_g.at[k, layer, :, cols], (ovg_ref, ovu_ref)[k].at[layer, :, cols], keep_v.at[q, k]).start()

    def down_own_step(layer, r, k):
        rows_k = pl.ds(k * half, half)
        starting = own_d.at[r, pl.ds(0, 2), rows_k]
        here, sums = arrived(slot_d.at[r, k], drs_got.at[r, k], drs_start.at[r, k], starting, k)
        part = got_d[z, rows_k].astype(F32) + own_d[r, z, rows_k].astype(F32)
        g = (sums + part).astype(BF).astype(F32)
        w1, m1, v1 = adamw(wo_d[layer, rows_k].astype(F32), m_d[layer, rows_k], v_d[layer, rows_k], g)
        m_d[layer, rows_k], v_d[layer, rows_k], here[...] = m1, v1, w1
        publish(
            here, nd_ref.at[layer, dblock_of(k, z)], dkeep_w.at[r, k],
            dag_send.at[r, k], dag_got.at[r, k], dfw_send.at[r, k], dfw_got.at[r, k], k,
        )
        pltpu.make_async_copy(m_d.at[layer, rows_k], omd_ref.at[layer, rows_k], dkeep_m.at[r, k]).start()
        pltpu.make_async_copy(v_d.at[layer, rows_k], ovd_ref.at[layer, rows_k], dkeep_v.at[r, k]).start()

    def hand_on(s, here_of, send, got, fsend, fgot, k):
        for way, length, base in ways[k]:

            @pl.when(s <= length)
            def _():
                here = here_of(going(way, s))
                pltpu.make_async_copy(here, here, got.at[base + s - 1]).wait()

                @pl.when(s < length)
                def _():
                    remote(here, here, send, got.at[base + s], near[way]).start()

                remote(here, here, fsend, fgot, mate).start()

    def gather_step(s, layer, j, q, k):
        cols, outs = strip_outs(layer, j)
        hand_on(
            s, lambda b: outs[k].at[layer, block_of(k, b), cols],
            ag_send.at[q, k], ag_got.at[q, k], fw_send.at[q, k], fw_got.at[q, k], k,
        )

    def down_gather_step(s, layer, r, k):
        hand_on(
            s, lambda b: nd_ref.at[layer, dblock_of(k, b)],
            dag_send.at[r, k], dag_got.at[r, k], dfw_send.at[r, k], dfw_got.at[r, k], k,
        )

    steps = 2 * far + 1
    per = POINTS // 2
    lags = -(-steps // per)

    def point(i, p):
        def advance(lag, k):
            g = i - lag
            r, j = g // turns, g % turns
            o = (lag - 1) * per + p // 2
            layer, q = top - r, r * STRIPS + j

            @pl.when((g >= 0) & (g <= last) & (j < STRIPS))
            def _():
                if k == 0:

                    @pl.when(o == 0)
                    def _():
                        pltpu.make_async_copy(got_g.at[j], got_g.at[j], pair_got.at[q]).wait()

                    @pl.when((o == 0) & (j == STRIPS - 1))
                    def _():
                        pltpu.make_async_copy(got_d, got_d, dpair_got.at[r]).wait()

                    @pl.when((o == far) & (g == 0))
                    def _():
                        for copy in params:
                            copy.wait()

                @pl.when(o < far)
                def _():
                    ring_step(o, layer, j, q, k)

                @pl.when(o == far)
                def _():
                    own_step(layer, j, q, k)

                @pl.when(o > far)
                def _():
                    gather_step(o - far, layer, j, q, k)

                @pl.when(j == STRIPS - 1)
                def _():
                    @pl.when(o < far)
                    def _():
                        dring_step(o, layer, r, k)

                    @pl.when(o == far)
                    def _():
                        down_own_step(layer, r, k)

                    @pl.when(o > far)
                    def _():
                        down_gather_step(o - far, layer, r, k)

                if k == 1:

                    @pl.when((o == far) & (r < layers - 1))
                    def _():
                        pl.semaphore_signal(credit, inc=1, device_id={"dp": mate}, device_id_type=MESH)

        for k in range(2):

            @pl.when(p % 2 == k)
            def _():
                def lag_step(idx, carry):
                    advance(lags - idx, k)
                    return carry

                lax.fori_loop(0, lags, lag_step, 0)

    def pair_copy(j, q):
        return remote(own_g.at[STRIPS + q % 2], got_g.at[j], pair_send.at[q], pair_got.at[q], mate)

    def dpair_copy(r):
        return remote(own_d.at[layers], got_d, dpair_send.at[r], dpair_got.at[r], mate)

    def segment(i, p):
        r, j = i // turns, i % turns
        q = r * STRIPS + j
        strip = (i <= last) & (j < STRIPS)

        @pl.when((i == 0) & (p == 0))
        def _():
            for k in (1, 2, 3):
                first[k].wait()

        @pl.when((i == turns) & (p == 0))
        def _():
            for k in range(4):
                second[k].wait()

        @pl.when(strip & (p < slabs))
        def _():
            strip_block(j, p)

        @pl.when((i == STRIPS - 1) & (p == slabs))
        def _():
            states.start()

        @pl.when((i == turns) & (p == slabs - 1))
        def _():
            second[4].wait()

        @pl.when(strip & (p == slabs - 1))
        def _():
            @pl.when(q >= 2)
            def _():
                pair_copy(j, q - 2).wait_send()

            @pl.when((r > 0) & (j == 0))
            def _():
                dpair_copy(r - 1).wait_send()

        @pl.when(strip & (p >= slabs - 1))
        def _():
            def one(e, carry):
                weight_rows(q, j, e // pieces, e % pieces)
                return carry

            ahead = p - (slabs - 1)
            lax.fori_loop(jnp.maximum(2 * ahead - 1, 0), jnp.minimum(2 * ahead + 1, 2 * pieces), one, 0)

        @pl.when(strip & (p == POINTS - 1))
        def _():
            @pl.when(r > 0)
            def _():
                pl.semaphore_wait(credit, 1)

            pair_copy(j, q).start()

            def one(e, carry):
                down_rows(r, j, e)
                return carry

            lax.fori_loop(0, pieces, one, 0)

            @pl.when(j == STRIPS - 1)
            def _():
                dpair_copy(r).start()

        @pl.when((i < last) & (j == STRIPS))
        def _():
            @pl.when(p == 0)
            def _():
                second[3].start()
                states.wait()

            def one(t, carry):
                state_block(t)
                return carry

            lax.fori_loop((p * blocks) // POINTS, ((p + 1) * blocks) // POINTS, one, 0)

            @pl.when(p == POINTS - 1)
            def _():
                for k in (0, 1, 2, 4):
                    second[k].start()

    def turn(i, carry):
        def part(p, carry):
            segment(i, p)
            point(i, p)
            return carry

        return lax.fori_loop(0, POINTS, part, carry)

    lax.fori_loop(0, last + 1 + lags, turn, 0)

    def all_of(ref, sem):
        pltpu.make_async_copy(ref, ref, sem).wait()

    def finish(q, carry):
        j = lax.rem(q, STRIPS)
        layer = top - q // STRIPS
        cols, outs = strip_outs(layer, j)

        @pl.when(q >= layers * STRIPS - 2)
        def _():
            pair_copy(j, q).wait_send()

        for k in range(2):
            all_of(slot_g.at[q, k, pl.ds(0, chips - 3)], rs_send.at[q, k])
            all_of(slot_g.at[q, k, pl.ds(0, chips - 1)], ag_send.at[q, k])
            all_of(got_g.at[j, k], fw_send.at[q, k])
            all_of(got_g.at[j, k], fw_got.at[q, k])
            all_of(slot_g.at[q, k, 0], keep_w.at[q, k])
            all_of(m_g.at[k, layer, :, cols], keep_m.at[q, k])
            all_of(v_g.at[k, layer, :, cols], keep_v.at[q, k])
        return carry

    lax.fori_loop(0, layers * STRIPS, finish, 0)
    for r in range(layers):
        layer = top - r
        if r == layers - 1:
            dpair_copy(r).wait_send()
        for k in range(2):
            part = pl.ds(k * half, half)
            all_of(slot_d.at[r, k, pl.ds(0, chips - 3)], drs_send.at[r, k])
            all_of(slot_d.at[r, k, pl.ds(0, chips - 1)], dag_send.at[r, k])
            all_of(got_d.at[:, part], dfw_send.at[r, k])
            all_of(got_d.at[:, part], dfw_got.at[r, k])
            all_of(slot_d.at[r, k, 0], dkeep_w.at[r, k])
            all_of(m_d.at[layer, part], dkeep_m.at[r, k])
            all_of(v_d.at[layer, part], dkeep_v.at[r, k])


def solution(mesh):
    n = mesh.shape["dp"]

    def body(x, dy, wg, wu, wd, mg, mu, md, vg, vu, vd):
        x, dy = x[0], dy[0]
        tokens, d = x.shape
        layers, _, ff = wg.shape
        chips, rows, drows = n // 2, d // n, ff // n
        half, width = drows // 2, ff // STRIPS
        tall, flat = jax.ShapeDtypeStruct((tokens, d), BF), jax.ShapeDtypeStruct((d, tokens), BF)
        sds = jax.ShapeDtypeStruct
        vm, sem = pltpu.VMEM, pltpu.SemaphoreType.DMA
        q, r = layers * STRIPS, layers
        scratch = [
            vm((tokens, d), BF), vm((d, tokens), BF), vm((tokens, d), BF), vm((d, tokens), BF),
            vm((d, ff), BF), vm((d, ff), BF), vm((ff, d), BF),
            vm((2, tokens, ff), BF), vm((tokens, width), BF),
            vm((STRIPS + 2, 2, chips, rows, width), BF), vm((STRIPS, 2, chips, rows, width), BF),
            vm((layers + 1, chips, drows, d), BF), vm((chips, drows, d), BF),
            vm((q, 2, chips - 1, rows, width), BF), vm((r, 2, chips - 1, half, d), BF),
            vm((2, layers, rows, ff), BF), vm((layers, drows, d), BF),
            vm((2, layers, rows, ff), F32), vm((2, layers, rows, ff), F32),
            vm((layers, drows, d), F32), vm((layers, drows, d), F32),
            sem((9,)), sem((tokens // BLOCK,)), sem((3,)), sem((9,)), sem((q,)), sem((q,)),
            sem((q, 2)), sem((q, 2)), sem((q, 2, chips - 1)), sem((q, 2)), sem((q, 2, chips - 1)), sem((q, 2)), sem((q, 2)),
            sem((q, 2)), sem((q, 2)), sem((q, 2)),
            sem((r,)), sem((r,)),
            sem((r, 2)), sem((r, 2)), sem((r, 2, chips - 1)), sem((r, 2)), sem((r, 2, chips - 1)), sem((r, 2)), sem((r, 2)),
            sem((r, 2)), sem((r, 2)), sem((r, 2)),
            pltpu.SemaphoreType.REGULAR,
        ]
        return pl.pallas_call(
            functools.partial(train, n),
            in_specs=[ANY] * 11,
            out_specs=[ANY] * 12,
            out_shape=[sds(t.shape, BF) for t in (wg, wu, wd)] + [sds(t.shape, F32) for t in (mg, mu, md, vg, vu, vd)] + [tall, tall, flat],
            scratch_shapes=scratch,
            compiler_params=pltpu.CompilerParams(
                collective_id=0, has_side_effects=True, vmem_limit_bytes=67_043_328
            ),
            name="step",
        )(x, dy, wg, wu, wd, mg, mu, md, vg, vu, vd)[:9]

    seq, whole, rows = P(("rep", "dp"), None, None), P(None, None, None), P(None, "dp", None)
    return jax.shard_map(
        body,
        mesh=mesh,
        in_specs=(seq, seq, whole, whole, whole) + (rows,) * 6,
        out_specs=(P("rep", None, None),) * 3 + (P("rep", "dp", None),) * 6,
        check_vma=False,
    )
```

```python
import functools

import jax
import jax.numpy as jnp
from jax import lax
from jax.experimental import pallas as pl
from jax.experimental.pallas import tpu as pltpu
from jax.sharding import PartitionSpec as P

MESH = pl.DeviceIdType.MESH
BF, F32 = jnp.bfloat16, jnp.float32
BLOCK = 512
TALL = 1024
STRIPS = 4
POINTS = 6
ANY = pl.BlockSpec(memory_space=pl.ANY)


def dot(a, b, dims=((1,), (0,))):
    return lax.dot_general(a, b, (dims, ((), ())), preferred_element_type=F32)


def scale_of(wide):
    return lax.rsqrt(jnp.mean(wide * wide, -1, keepdims=True) + 1e-6)


def adamw(w, m, v, g):
    m = 0.9 * m + 0.1 * g
    v = 0.95 * v + 0.05 * g * g
    step = m * lax.rsqrt(v + 1e-8) + 0.1 * w
    return (w - 0.02 * step).astype(BF), m, v


def train(
    n, x_ref, dyi_ref, wg_ref, wu_ref, wd_ref,
    mg_ref, mu_ref, md_ref, vg_ref, vu_ref, vd_ref,
    ng_ref, nu_ref, nd_ref, omg_ref, omu_ref, omd_ref, ovg_ref, ovu_ref, ovd_ref, h_ref, a_ref, at_ref,
    act, actt, dy, dyt, wg, wu, wd, dgu, prod, own_g, got_g, own_d, got_d, slot_g, slot_d,
    wo_g, wo_d, m_g, v_g, m_d, v_d,
    load, x_load, first_out, opt_load, pair_send, pair_got, rs_start, rs_send, rs_got, ag_send, ag_got, fw_send, fw_got, keep_w, keep_m, keep_v,
    dpair_send, dpair_got, drs_start, drs_send, drs_got, dag_send, dag_got, dfw_send, dfw_got, dkeep_w, dkeep_m, dkeep_v, credit, dcredit,
):
    chips = n // 2
    tokens, d = dy.shape
    ff = wg.shape[1]
    width = ff // STRIPS
    rows, drows = d // n, ff // n
    half = drows // 2
    layers = wg_ref.shape[0]
    blocks = tokens // BLOCK
    turns = STRIPS + 1
    last = layers * turns - 2

    me = lax.axis_index("dp")
    z, c = me // 2, me % 2
    near = (((z + 1) % chips) * 2 + c, ((z + chips - 1) % chips) * 2 + c)
    mate = z * 2 + (1 - c)

    barrier = pltpu.get_barrier_semaphore()
    for other in (*near, mate):
        pl.semaphore_signal(barrier, inc=1, device_id={"dp": other}, device_id_type=MESH)
    pl.semaphore_wait(barrier, 3)

    def fetch(src, dst, k):
        return pltpu.make_async_copy(src, dst, load.at[k])

    top = layers - 1

    def tok(t):
        return pl.ds(pl.multiple_of(t * BLOCK, BLOCK), BLOCK)

    def loads(layer, acts, actst):
        return (
            fetch(acts, act, 0), fetch(wg_ref.at[layer], wg, 1), fetch(wu_ref.at[layer], wu, 2),
            fetch(wd_ref.at[layer], wd, 3), fetch(actst, actt, 4),
        )

    wg_v, wu_v, at_v = (dgu.at[0, pl.ds(k * d, d)] for k in range(3))
    wd_v, x_v, h_v = (dgu.at[1, :, pl.ds(k * d, d)] for k in range(3))

    def x_copy(t):
        return pltpu.make_async_copy(x_ref.at[tok(t)], x_v.at[tok(t)], x_load.at[t])

    early = (fetch(wg_ref.at[0], wg_v, 5), fetch(wu_ref.at[0], wu_v, 6), fetch(wd_ref.at[0], wd_v, 7), fetch(dyi_ref, dy, 8))
    first = (None, fetch(wg_ref.at[top], wg, 1), fetch(wu_ref.at[top], wu, 2), fetch(wd_ref.at[top], wd, 3))
    x_copy(0).start()
    for copy in early:
        copy.start()
    for t in range(1, blocks):
        x_copy(t).start()
    for copy in first[1:]:
        copy.start()
    mine = pl.ds(pl.multiple_of(me * rows, 8), rows)
    dmine = pl.ds(pl.multiple_of(me * drows, 8), drows)
    params = [
        (wg_ref.at[:, mine], wo_g.at[0]), (wu_ref.at[:, mine], wo_g.at[1]), (wd_ref.at[:, dmine], wo_d),
        (mg_ref, m_g.at[0]), (mu_ref, m_g.at[1]), (md_ref, m_d),
        (vg_ref, v_g.at[0]), (vu_ref, v_g.at[1]), (vd_ref, v_d),
    ]
    params = [pltpu.make_async_copy(s, t, opt_load.at[k]) for k, (s, t) in enumerate(params)]
    for copy in params:
        copy.start()

    second = loads(0, a_ref, at_ref)
    states = fetch(h_ref, act, 0)

    def remote(src, dst, send, got, to):
        return pltpu.make_async_remote_copy(src, dst, send, got, device_id={"dp": to}, device_id_type=MESH)

    def first_outs(part):
        return (
            pltpu.make_async_copy(x_v.at[part], a_ref.at[part], first_out.at[0]),
            pltpu.make_async_copy(at_v.at[:, part], at_ref.at[:, part], first_out.at[1]),
            pltpu.make_async_copy(h_v.at[part], h_ref.at[part], first_out.at[2]),
        )

    def forward_block(t):
        x_copy(t).wait()
        part = tok(t)
        wide = x_v[part, :].astype(F32)
        a = wide * scale_of(wide)
        at_v[:, part] = a.T.astype(BF)
        a = a.astype(BF)
        for j in range(STRIPS):
            cols = slice(j * width, (j + 1) * width)
            gate, up = dot(a, wg_v[:, cols]), dot(a, wu_v[:, cols])
            prod[j * BLOCK : (j + 1) * BLOCK, :] = (gate * jax.nn.sigmoid(gate) * up).astype(BF)

        @pl.when(t == 0)
        def _():
            early[2].wait()
            early[3].wait()

        down = sum(
            dot(prod[j * BLOCK : (j + 1) * BLOCK, :], wd_v[j * width : (j + 1) * width, :]) for j in range(STRIPS)
        ).astype(BF)
        h = (wide + down.astype(F32)).astype(BF)
        x_v[part, :] = a
        h_v[part, :] = h
        wide = h.astype(F32)
        b = wide * scale_of(wide)
        actt[:, part] = b.T.astype(BF)
        act[part, :] = b.astype(BF)
        dyt[:, part] = dy[part, :].astype(F32).T.astype(BF)
        for copy in first_outs(part):
            copy.start()

    early[0].wait()
    early[1].wait()

    def forward_step(t, carry):
        forward_block(t)
        return carry

    lax.fori_loop(0, blocks, forward_step, 0)
    for copy in first_outs(pl.ds(0, tokens)):
        copy.wait()

    pieces = width // 256
    slabs = tokens // TALL * pieces

    def strip_block(j, e):
        rows_e = pl.ds(pl.multiple_of(e // pieces * TALL, TALL), TALL)
        cols = pl.ds(pl.multiple_of(j * width + e % pieces * 256, 256), 256)
        here = pl.ds(pl.multiple_of(e % pieces * 256, 256), 256)
        a = act[rows_e, :]
        gate = dot(a, wg[:, cols])
        up = dot(a, wu[:, cols])
        dact = dot(dy[rows_e, :], wd[cols, :], ((1,), (1,))).astype(BF).astype(F32)
        sig = jax.nn.sigmoid(gate)
        silu = gate * sig
        prod[rows_e, here] = (silu * up).astype(BF)
        dgu[0, rows_e, cols] = (dact * up * (sig + silu * (1.0 - sig))).astype(BF)
        dgu[1, rows_e, cols] = (dact * silu).astype(BF)

    def weight_rows(q, j, k, piece):
        cols = pl.ds(pl.multiple_of(j * width + piece * 256, 256), 256)
        out = pl.ds(pl.multiple_of(piece * 256, 256), 256)
        total = dot(actt[...], dgu[k, :, cols])
        for chip in range(chips):
            for core in range(2):
                at = (chip * 2 + core) * rows
                own_g[jnp.where(c == core, j, STRIPS + q % 2), k, chip, :, out] = total[at : at + rows].astype(BF)

    def down_rows(r, j, piece):
        total = dot(dyt[...], prod[:, pl.ds(pl.multiple_of(piece * 256, 256), 256)])
        total = total.T.astype(BF)
        per = 256 // (2 * drows)
        for k in range(per):
            for core in range(2):
                at = (k * 2 + core) * drows
                own_d[jnp.where(c == core, r, layers), (j * pieces + piece) * per + k] = total[at : at + drows]

    def state_block(t):
        by_gate = dot(dgu[0, tok(t), :], wg[...], ((1,), (1,))).astype(BF)
        by_up = dot(dgu[1, tok(t), :], wu[...], ((1,), (1,))).astype(BF)
        by_a = (by_gate.astype(F32) + by_up.astype(F32)).astype(BF).astype(F32)
        wide = act[tok(t), :].astype(F32)
        scale = scale_of(wide)
        lean = jnp.mean(by_a * wide, -1, keepdims=True)
        by_h = (by_a * scale - wide * (scale * scale * scale * lean)).astype(BF)
        total = dy[tok(t), :].astype(F32) + by_h.astype(F32)
        dy[tok(t), :] = total.astype(BF)
        dyt[:, tok(t)] = total.astype(BF).astype(F32).T.astype(BF)

    def strip_outs(layer, j):
        return pl.ds(pl.multiple_of(j * width, width), width), (ng_ref, nu_ref)

    def block_of(k, chip):
        return pl.ds(pl.multiple_of((chip * 2 + c) * rows, 8), rows)

    def dblock_of(k, chip):
        return pl.ds(pl.multiple_of((chip * 2 + c) * drows + k * half, 8), half)

    def wrap(v):
        return lax.rem(v + 2 * chips, chips)

    far = chips // 2
    ways = [((0, far - k, 0), (1, chips - 1 - (far - k), far - k)) for k in range(2)]

    def coming(way, length, o):
        return wrap(z + length - o) if way == 0 else wrap(z - length + o)

    def going(way, s):
        return wrap(z - s) if way == 0 else wrap(z + s)

    def ring_step(o, layer, j, q, k):
        for way, length, base in ways[k]:

            @pl.when(o < length)
            def _():
                b = coming(way, length, o)
                own = own_g.at[j, k, b]
                part = got_g[j, k, b].astype(F32) + own[...].astype(F32)

                @pl.when(o == 0)
                def _():
                    own[...] = part.astype(BF)
                    remote(own, slot_g.at[q, k, base], rs_start.at[q, k], rs_got.at[q, k, base], near[way]).start()

                @pl.when(o > 0)
                def _():
                    here = slot_g.at[q, k, base + o - 1]
                    pltpu.make_async_copy(here, here, rs_got.at[q, k, base + o - 1]).wait()
                    here[...] = (here[...].astype(F32) + part).astype(BF)
                    remote(here, slot_g.at[q, k, base + o], rs_send.at[q, k], rs_got.at[q, k, base + o], near[way]).start()

    def dring_step(o, layer, r, k):
        rows_k = pl.ds(k * half, half)
        for way, length, base in ways[k]:

            @pl.when(o < length)
            def _():
                b = coming(way, length, o)
                own = own_d.at[r, b, rows_k]
                part = got_d[b, rows_k].astype(F32) + own[...].astype(F32)

                @pl.when(o == 0)
                def _():
                    own[...] = part.astype(BF)
                    remote(own, slot_d.at[r, k, base], drs_start.at[r, k], drs_got.at[r, k, base], near[way]).start()

                @pl.when(o > 0)
                def _():
                    here = slot_d.at[r, k, base + o - 1]
                    pltpu.make_async_copy(here, here, drs_got.at[r, k, base + o - 1]).wait()
                    here[...] = (here[...].astype(F32) + part).astype(BF)
                    remote(here, slot_d.at[r, k, base + o], drs_send.at[r, k], drs_got.at[r, k, base + o], near[way]).start()

    def publish(src, dst, keep, send, got, fsend, fgot, k):
        pltpu.make_async_copy(src, dst, keep).start()
        for way, _, base in ways[k]:
            remote(src, dst, send, got.at[base], near[way]).start()
        remote(src, dst, fsend, fgot, mate).start()

    def arrived(slots, sems, starts, starting, k):
        pltpu.make_async_copy(starting, starting, starts).wait()
        first, second = (slots.at[base + length - 1] for _, length, base in ways[k])
        for (_, length, base), here in zip(ways[k], (first, second)):
            pltpu.make_async_copy(here, here, sems.at[base + length - 1]).wait()
        return first, first[...].astype(F32) + second[...].astype(F32)

    def own_step(layer, j, q, k):
        cols, outs = strip_outs(layer, j)
        here, sums = arrived(slot_g.at[q, k], rs_got.at[q, k], rs_start.at[q, k], own_g.at[j, k, pl.ds(0, 2)], k)
        part = got_g[j, k, z].astype(F32) + own_g[j, k, z].astype(F32)
        g = (sums + part).astype(BF).astype(F32)
        w1, m1, v1 = adamw(wo_g[k, layer, :, cols].astype(F32), m_g[k, layer, :, cols], v_g[k, layer, :, cols], g)
        m_g[k, layer, :, cols], v_g[k, layer, :, cols], here[...] = m1, v1, w1
        publish(
            here, outs[k].at[layer, block_of(k, z), cols], keep_w.at[q, k],
            ag_send.at[q, k], ag_got.at[q, k], fw_send.at[q, k], fw_got.at[q, k], k,
        )
        pltpu.make_async_copy(m_g.at[k, layer, :, cols], (omg_ref, omu_ref)[k].at[layer, :, cols], keep_m.at[q, k]).start()
        pltpu.make_async_copy(v_g.at[k, layer, :, cols], (ovg_ref, ovu_ref)[k].at[layer, :, cols], keep_v.at[q, k]).start()

    def down_own_step(layer, r, k):
        rows_k = pl.ds(k * half, half)
        starting = own_d.at[r, pl.ds(0, 2), rows_k]
        here, sums = arrived(slot_d.at[r, k], drs_got.at[r, k], drs_start.at[r, k], starting, k)
        part = got_d[z, rows_k].astype(F32) + own_d[r, z, rows_k].astype(F32)
        g = (sums + part).astype(BF).astype(F32)
        w1, m1, v1 = adamw(wo_d[layer, rows_k].astype(F32), m_d[layer, rows_k], v_d[layer, rows_k], g)
        m_d[layer, rows_k], v_d[layer, rows_k], here[...] = m1, v1, w1
        publish(
            here, nd_ref.at[layer, dblock_of(k, z)], dkeep_w.at[r, k],
            dag_send.at[r, k], dag_got.at[r, k], dfw_send.at[r, k], dfw_got.at[r, k], k,
        )
        pltpu.make_async_copy(m_d.at[layer, rows_k], omd_ref.at[layer, rows_k], dkeep_m.at[r, k]).start()
        pltpu.make_async_copy(v_d.at[layer, rows_k], ovd_ref.at[layer, rows_k], dkeep_v.at[r, k]).start()

    def hand_on(s, here_of, send, got, fsend, fgot, k):
        for way, length, base in ways[k]:

            @pl.when(s <= length)
            def _():
                here = here_of(going(way, s))
                pltpu.make_async_copy(here, here, got.at[base + s - 1]).wait()

                @pl.when(s < length)
                def _():
                    remote(here, here, send, got.at[base + s], near[way]).start()

                remote(here, here, fsend, fgot, mate).start()

    def gather_step(s, layer, j, q, k):
        cols, outs = strip_outs(layer, j)
        hand_on(
            s, lambda b: outs[k].at[layer, block_of(k, b), cols],
            ag_send.at[q, k], ag_got.at[q, k], fw_send.at[q, k], fw_got.at[q, k], k,
        )

    def down_gather_step(s, layer, r, k):
        hand_on(
            s, lambda b: nd_ref.at[layer, dblock_of(k, b)],
            dag_send.at[r, k], dag_got.at[r, k], dfw_send.at[r, k], dfw_got.at[r, k], k,
        )

    steps = 2 * far + 1
    per = POINTS // 2
    lags = -(-steps // per)

    def point(i, p):
        def advance(lag, k):
            g = i - lag
            r, j = g // turns, g % turns
            o = (lag - 1) * per + p // 2
            layer, q = top - r, r * STRIPS + j

            @pl.when((g >= 0) & (g <= last) & (j < STRIPS))
            def _():
                if k == 0:

                    @pl.when(o == 0)
                    def _():
                        pltpu.make_async_copy(got_g.at[j], got_g.at[j], pair_got.at[q]).wait()

                    @pl.when((o == far) & (g == 0))
                    def _():
                        for copy in params:
                            copy.wait()

                @pl.when(o < far)
                def _():
                    ring_step(o, layer, j, q, k)

                @pl.when(o == far)
                def _():
                    own_step(layer, j, q, k)

                @pl.when(o > far)
                def _():
                    gather_step(o - far, layer, j, q, k)

                if k == 1:

                    @pl.when((o == far) & (r < layers - 1))
                    def _():
                        pl.semaphore_signal(credit, inc=1, device_id={"dp": mate}, device_id_type=MESH)

        def down_advance(lag, k):
            g = i - lag
            r, j = g // turns, g % turns
            slow = r < layers - 1
            o = jnp.where(slow, (lag - 1) * 2, (lag - 1) * per) + p // 2
            layer = top - r
            go = (g >= 0) & (g <= last) & (j == STRIPS - 1) & (o < steps) & (p // 2 < jnp.where(slow, 2, per))

            @pl.when(go)
            def _():
                if k == 0:

                    @pl.when(o == 0)
                    def _():
                        pltpu.make_async_copy(got_d, got_d, dpair_got.at[r]).wait()

                @pl.when(o < far)
                def _():
                    dring_step(o, layer, r, k)

                @pl.when(o == far)
                def _():
                    down_own_step(layer, r, k)

                @pl.when(o > far)
                def _():
                    down_gather_step(o - far, layer, r, k)

                if k == 1:

                    @pl.when((o == far) & slow)
                    def _():
                        pl.semaphore_signal(dcredit, inc=1, device_id={"dp": mate}, device_id_type=MESH)

        for k in range(2):

            @pl.when(p % 2 == k)
            def _():
                def lag_step(idx, carry):
                    advance(lags - idx, k)
                    return carry

                lax.fori_loop(0, lags, lag_step, 0)

                def down_lag_step(idx, carry):
                    down_advance(1 + idx, k)
                    return carry

                lax.fori_loop(0, -(-steps // 2), down_lag_step, 0)

    def pair_copy(j, q):
        return remote(own_g.at[STRIPS + q % 2], got_g.at[j], pair_send.at[q], pair_got.at[q], mate)

    def dpair_copy(r):
        return remote(own_d.at[layers], got_d, dpair_send.at[r], dpair_got.at[r], mate)

    def segment(i, p):
        r, j = i // turns, i % turns
        q = r * STRIPS + j
        strip = (i <= last) & (j < STRIPS)

        @pl.when((i == 0) & (p == 0))
        def _():
            for k in (1, 2, 3):
                first[k].wait()

        @pl.when((i == turns) & (p == 0))
        def _():
            for k in range(4):
                second[k].wait()

        @pl.when(strip & (p < slabs))
        def _():
            strip_block(j, p)

        @pl.when((i == STRIPS - 1) & (p == slabs))
        def _():
            states.start()

        @pl.when((i == turns) & (p == slabs - 1))
        def _():
            second[4].wait()

        @pl.when(strip & (p == slabs - 1))
        def _():
            @pl.when(q >= 2)
            def _():
                pair_copy(j, q - 2).wait_send()

            @pl.when((r > 0) & (j == 0))
            def _():
                dpair_copy(r - 1).wait_send()

        @pl.when(strip & (p >= slabs - 1))
        def _():
            def one(e, carry):
                weight_rows(q, j, e // pieces, e % pieces)
                return carry

            ahead = p - (slabs - 1)
            lax.fori_loop(jnp.maximum(2 * ahead - 1, 0), jnp.minimum(2 * ahead + 1, 2 * pieces), one, 0)

        @pl.when(strip & (p == POINTS - 1))
        def _():
            @pl.when(r > 0)
            def _():
                pl.semaphore_wait(credit, 1)

            pair_copy(j, q).start()

            def one(e, carry):
                down_rows(r, j, e)
                return carry

            lax.fori_loop(0, pieces, one, 0)

            @pl.when(j == STRIPS - 1)
            def _():
                @pl.when(r > 0)
                def _():
                    pl.semaphore_wait(dcredit, 1)

                dpair_copy(r).start()

        @pl.when((i < last) & (j == STRIPS))
        def _():
            @pl.when(p == 0)
            def _():
                second[3].start()
                states.wait()

            def one(t, carry):
                state_block(t)
                return carry

            lax.fori_loop((p * blocks) // POINTS, ((p + 1) * blocks) // POINTS, one, 0)

            @pl.when(p == POINTS - 1)
            def _():
                for k in (0, 1, 2, 4):
                    second[k].start()

    def turn(i, carry):
        def part(p, carry):
            segment(i, p)
            point(i, p)
            return carry

        return lax.fori_loop(0, POINTS, part, carry)

    lax.fori_loop(0, last + 1 + lags, turn, 0)

    def all_of(ref, sem):
        pltpu.make_async_copy(ref, ref, sem).wait()

    def finish(q, carry):
        j = lax.rem(q, STRIPS)
        layer = top - q // STRIPS
        cols, outs = strip_outs(layer, j)

        @pl.when(q >= layers * STRIPS - 2)
        def _():
            pair_copy(j, q).wait_send()

        for k in range(2):
            all_of(slot_g.at[q, k, pl.ds(0, chips - 3)], rs_send.at[q, k])
            all_of(slot_g.at[q, k, pl.ds(0, chips - 1)], ag_send.at[q, k])
            all_of(got_g.at[j, k], fw_send.at[q, k])
            all_of(got_g.at[j, k], fw_got.at[q, k])
            all_of(slot_g.at[q, k, 0], keep_w.at[q, k])
            all_of(m_g.at[k, layer, :, cols], keep_m.at[q, k])
            all_of(v_g.at[k, layer, :, cols], keep_v.at[q, k])
        return carry

    lax.fori_loop(0, layers * STRIPS, finish, 0)
    for r in range(layers):
        layer = top - r
        if r == layers - 1:
            dpair_copy(r).wait_send()
        for k in range(2):
            part = pl.ds(k * half, half)
            all_of(slot_d.at[r, k, pl.ds(0, chips - 3)], drs_send.at[r, k])
            all_of(slot_d.at[r, k, pl.ds(0, chips - 1)], dag_send.at[r, k])
            all_of(got_d.at[:, part], dfw_send.at[r, k])
            all_of(got_d.at[:, part], dfw_got.at[r, k])
            all_of(slot_d.at[r, k, 0], dkeep_w.at[r, k])
            all_of(m_d.at[layer, part], dkeep_m.at[r, k])
            all_of(v_d.at[layer, part], dkeep_v.at[r, k])


def solution(mesh):
    n = mesh.shape["dp"]

    def body(x, dy, wg, wu, wd, mg, mu, md, vg, vu, vd):
        x, dy = x[0], dy[0]
        tokens, d = x.shape
        layers, _, ff = wg.shape
        chips, rows, drows = n // 2, d // n, ff // n
        half, width = drows // 2, ff // STRIPS
        tall, flat = jax.ShapeDtypeStruct((tokens, d), BF), jax.ShapeDtypeStruct((d, tokens), BF)
        sds = jax.ShapeDtypeStruct
        vm, sem = pltpu.VMEM, pltpu.SemaphoreType.DMA
        q, r = layers * STRIPS, layers
        scratch = [
            vm((tokens, d), BF), vm((d, tokens), BF), vm((tokens, d), BF), vm((d, tokens), BF),
            vm((d, ff), BF), vm((d, ff), BF), vm((ff, d), BF),
            vm((2, tokens, ff), BF), vm((tokens, width), BF),
            vm((STRIPS + 2, 2, chips, rows, width), BF), vm((STRIPS, 2, chips, rows, width), BF),
            vm((layers + 1, chips, drows, d), BF), vm((chips, drows, d), BF),
            vm((q, 2, chips - 1, rows, width), BF), vm((r, 2, chips - 1, half, d), BF),
            vm((2, layers, rows, ff), BF), vm((layers, drows, d), BF),
            vm((2, layers, rows, ff), F32), vm((2, layers, rows, ff), F32),
            vm((layers, drows, d), F32), vm((layers, drows, d), F32),
            sem((9,)), sem((tokens // BLOCK,)), sem((3,)), sem((9,)), sem((q,)), sem((q,)),
            sem((q, 2)), sem((q, 2)), sem((q, 2, chips - 1)), sem((q, 2)), sem((q, 2, chips - 1)), sem((q, 2)), sem((q, 2)),
            sem((q, 2)), sem((q, 2)), sem((q, 2)),
            sem((r,)), sem((r,)),
            sem((r, 2)), sem((r, 2)), sem((r, 2, chips - 1)), sem((r, 2)), sem((r, 2, chips - 1)), sem((r, 2)), sem((r, 2)),
            sem((r, 2)), sem((r, 2)), sem((r, 2)),
            pltpu.SemaphoreType.REGULAR, pltpu.SemaphoreType.REGULAR,
        ]
        return pl.pallas_call(
            functools.partial(train, n),
            in_specs=[ANY] * 11,
            out_specs=[ANY] * 12,
            out_shape=[sds(t.shape, BF) for t in (wg, wu, wd)] + [sds(t.shape, F32) for t in (mg, mu, md, vg, vu, vd)] + [tall, tall, flat],
            scratch_shapes=scratch,
            compiler_params=pltpu.CompilerParams(
                collective_id=0, has_side_effects=True, vmem_limit_bytes=67_043_328
            ),
            name="step",
        )(x, dy, wg, wu, wd, mg, mu, md, vg, vu, vd)[:9]

    seq, whole, rows = P(("rep", "dp"), None, None), P(None, None, None), P(None, "dp", None)
    return jax.shard_map(
        body,
        mesh=mesh,
        in_specs=(seq, seq, whole, whole, whole) + (rows,) * 6,
        out_specs=(P("rep", None, None),) * 3 + (P("rep", "dp", None),) * 6,
        check_vma=False,
    )
```

```python
import functools

import jax
import jax.numpy as jnp
from jax import lax
from jax.experimental import pallas as pl
from jax.experimental.pallas import tpu as pltpu
from jax.sharding import PartitionSpec as P

MESH = pl.DeviceIdType.MESH
BF, F32 = jnp.bfloat16, jnp.float32
BLOCK = 512
TALL = 1024
STRIPS = 4
POINTS = 6
ANY = pl.BlockSpec(memory_space=pl.ANY)


def dot(a, b, dims=((1,), (0,))):
    return lax.dot_general(a, b, (dims, ((), ())), preferred_element_type=F32)


def scale_of(wide):
    return lax.rsqrt(jnp.mean(wide * wide, -1, keepdims=True) + 1e-6)


def adamw(w, m, v, g):
    m = 0.9 * m + 0.1 * g
    v = 0.95 * v + 0.05 * g * g
    step = m * lax.rsqrt(v + 1e-8) + 0.1 * w
    return (w - 0.02 * step).astype(BF), m, v


def train(
    n, x_ref, dyi_ref, wg_ref, wu_ref, wd_ref,
    mg_ref, mu_ref, md_ref, vg_ref, vu_ref, vd_ref,
    ng_ref, nu_ref, nd_ref, omg_ref, omu_ref, omd_ref, ovg_ref, ovu_ref, ovd_ref, h_ref, a_ref, at_ref,
    act, actt, dy, dyt, wg, wu, wd, dgu, prod, own_g, got_g, own_d, got_d, slot_g, slot_d,
    wo_g, wo_d, m_g, v_g, m_d, v_d,
    load, x_load, first_out, opt_load, pair_send, pair_got, rs_start, rs_send, rs_got, ag_send, ag_got, fw_send, fw_got, keep_w, keep_m, keep_v,
    dpair_send, dpair_got, drs_start, drs_send, drs_got, dag_send, dag_got, dfw_send, dfw_got, dkeep_w, dkeep_m, dkeep_v, credit,
):
    chips = n // 2
    tokens, d = dy.shape
    ff = wg.shape[1]
    width = ff // STRIPS
    rows, drows = d // n, ff // n
    half = drows // 2
    layers = wg_ref.shape[0]
    blocks = tokens // BLOCK
    turns = STRIPS + 1
    last = layers * turns - 2

    me = lax.axis_index("dp")
    z, c = me // 2, me % 2
    near = (((z + 1) % chips) * 2 + c, ((z + chips - 1) % chips) * 2 + c)
    mate = z * 2 + (1 - c)

    barrier = pltpu.get_barrier_semaphore()
    for other in (*near, mate):
        pl.semaphore_signal(barrier, inc=1, device_id={"dp": other}, device_id_type=MESH)
    pl.semaphore_wait(barrier, 3)

    def fetch(src, dst, k):
        return pltpu.make_async_copy(src, dst, load.at[k])

    top = layers - 1

    def tok(t):
        return pl.ds(pl.multiple_of(t * BLOCK, BLOCK), BLOCK)

    def loads(layer, acts, actst):
        return (
            fetch(acts, act, 0), fetch(wg_ref.at[layer], wg, 1), fetch(wu_ref.at[layer], wu, 2),
            fetch(wd_ref.at[layer], wd, 3), fetch(actst, actt, 4),
        )

    wg_v, wu_v, at_v = (dgu.at[0, pl.ds(k * d, d)] for k in range(3))
    wd_v, x_v, h_v = (dgu.at[1, :, pl.ds(k * d, d)] for k in range(3))

    def x_copy(t):
        return pltpu.make_async_copy(x_ref.at[tok(t)], x_v.at[tok(t)], x_load.at[t])

    early = (fetch(wg_ref.at[0], wg_v, 5), fetch(wu_ref.at[0], wu_v, 6), fetch(wd_ref.at[0], wd_v, 7), fetch(dyi_ref, dy, 8))
    first = (None, fetch(wg_ref.at[top], wg, 1), fetch(wu_ref.at[top], wu, 2), fetch(wd_ref.at[top], wd, 3))
    x_copy(0).start()
    for copy in early:
        copy.start()
    for t in range(1, blocks):
        x_copy(t).start()
    for copy in first[1:]:
        copy.start()
    mine = pl.ds(pl.multiple_of(me * rows, 8), rows)
    dmine = pl.ds(pl.multiple_of(me * drows, 8), drows)
    params = [
        (wg_ref.at[:, mine], wo_g.at[0]), (wu_ref.at[:, mine], wo_g.at[1]), (wd_ref.at[:, dmine], wo_d),
        (mg_ref, m_g.at[0]), (mu_ref, m_g.at[1]), (md_ref, m_d),
        (vg_ref, v_g.at[0]), (vu_ref, v_g.at[1]), (vd_ref, v_d),
    ]
    params = [pltpu.make_async_copy(s, t, opt_load.at[k]) for k, (s, t) in enumerate(params)]
    for copy in params:
        copy.start()

    second = loads(0, a_ref, at_ref)
    states = fetch(h_ref, act, 0)

    def remote(src, dst, send, got, to):
        return pltpu.make_async_remote_copy(src, dst, send, got, device_id={"dp": to}, device_id_type=MESH)

    def first_outs(part):
        return (
            pltpu.make_async_copy(x_v.at[part], a_ref.at[part], first_out.at[0]),
            pltpu.make_async_copy(at_v.at[:, part], at_ref.at[:, part], first_out.at[1]),
            pltpu.make_async_copy(h_v.at[part], h_ref.at[part], first_out.at[2]),
        )

    def forward_block(t):
        x_copy(t).wait()
        part = tok(t)
        wide = x_v[part, :].astype(F32)
        a = wide * scale_of(wide)
        at_v[:, part] = a.T.astype(BF)
        a = a.astype(BF)
        for j in range(STRIPS):
            cols = slice(j * width, (j + 1) * width)
            gate, up = dot(a, wg_v[:, cols]), dot(a, wu_v[:, cols])
            prod[j * BLOCK : (j + 1) * BLOCK, :] = (gate * jax.nn.sigmoid(gate) * up).astype(BF)

        @pl.when(t == 0)
        def _():
            early[2].wait()
            early[3].wait()

        down = sum(
            dot(prod[j * BLOCK : (j + 1) * BLOCK, :], wd_v[j * width : (j + 1) * width, :]) for j in range(STRIPS)
        ).astype(BF)
        h = (wide + down.astype(F32)).astype(BF)
        x_v[part, :] = a
        h_v[part, :] = h
        wide = h.astype(F32)
        b = wide * scale_of(wide)
        actt[:, part] = b.T.astype(BF)
        act[part, :] = b.astype(BF)
        dyt[:, part] = dy[part, :].astype(F32).T.astype(BF)
        for copy in first_outs(part):
            copy.start()

    early[0].wait()
    early[1].wait()

    def forward_step(t, carry):
        forward_block(t)
        return carry

    lax.fori_loop(0, blocks, forward_step, 0)
    for copy in first_outs(pl.ds(0, tokens)):
        copy.wait()

    pieces = width // 256
    slabs = tokens // TALL * pieces

    def strip_block(j, e):
        rows_e = pl.ds(pl.multiple_of(e // pieces * TALL, TALL), TALL)
        cols = pl.ds(pl.multiple_of(j * width + e % pieces * 256, 256), 256)
        here = pl.ds(pl.multiple_of(e % pieces * 256, 256), 256)
        a = act[rows_e, :]
        gate = dot(a, wg[:, cols])
        up = dot(a, wu[:, cols])
        dact = dot(dy[rows_e, :], wd[cols, :], ((1,), (1,))).astype(BF).astype(F32)
        sig = jax.nn.sigmoid(gate)
        silu = gate * sig
        prod[rows_e, here] = (silu * up).astype(BF)
        dgu[0, rows_e, cols] = (dact * up * (sig + silu * (1.0 - sig))).astype(BF)
        dgu[1, rows_e, cols] = (dact * silu).astype(BF)

    def weight_rows(q, j, k, piece):
        cols = pl.ds(pl.multiple_of(j * width + piece * 256, 256), 256)
        out = pl.ds(pl.multiple_of(piece * 256, 256), 256)
        total = dot(actt[...], dgu[k, :, cols])
        for chip in range(chips):
            for core in range(2):
                at = (chip * 2 + core) * rows
                own_g[jnp.where(c == core, j, STRIPS + q % 2), k, chip, :, out] = total[at : at + rows].astype(BF)

    def down_rows(r, j, piece):
        total = dot(dyt[...], prod[:, pl.ds(pl.multiple_of(piece * 256, 256), 256)])
        total = total.T.astype(BF)
        per = 256 // (2 * drows)
        for k in range(per):
            for core in range(2):
                at = (k * 2 + core) * drows
                own_d[jnp.where(c == core, r, layers), (j * pieces + piece) * per + k] = total[at : at + drows]

    def state_block(t):
        by_gate = dot(dgu[0, tok(t), :], wg[...], ((1,), (1,))).astype(BF)
        by_up = dot(dgu[1, tok(t), :], wu[...], ((1,), (1,))).astype(BF)
        by_a = (by_gate.astype(F32) + by_up.astype(F32)).astype(BF).astype(F32)
        wide = act[tok(t), :].astype(F32)
        scale = scale_of(wide)
        lean = jnp.mean(by_a * wide, -1, keepdims=True)
        by_h = (by_a * scale - wide * (scale * scale * scale * lean)).astype(BF)
        total = dy[tok(t), :].astype(F32) + by_h.astype(F32)
        dy[tok(t), :] = total.astype(BF)
        dyt[:, tok(t)] = total.astype(BF).astype(F32).T.astype(BF)

    def strip_outs(layer, j):
        return pl.ds(pl.multiple_of(j * width, width), width), (ng_ref, nu_ref)

    def block_of(k, chip):
        return pl.ds(pl.multiple_of((chip * 2 + c) * rows, 8), rows)

    def dblock_of(k, chip):
        return pl.ds(pl.multiple_of((chip * 2 + c) * drows + k * half, 8), half)

    def wrap(v):
        return lax.rem(v + 2 * chips, chips)

    far = chips // 2
    ways = [((0, far - k, 0), (1, chips - 1 - (far - k), far - k)) for k in range(2)]

    def coming(way, length, o):
        return wrap(z + length - o) if way == 0 else wrap(z - length + o)

    def going(way, s):
        return wrap(z - s) if way == 0 else wrap(z + s)

    def ring_step(o, layer, j, q, k):
        for way, length, base in ways[k]:

            @pl.when(o < length)
            def _():
                b = coming(way, length, o)
                own = own_g.at[j, k, b]
                part = got_g[j, k, b].astype(F32) + own[...].astype(F32)

                @pl.when(o == 0)
                def _():
                    own[...] = part.astype(BF)
                    remote(own, slot_g.at[q, k, base], rs_start.at[q, k], rs_got.at[q, k, base], near[way]).start()

                @pl.when(o > 0)
                def _():
                    here = slot_g.at[q, k, base + o - 1]
                    pltpu.make_async_copy(here, here, rs_got.at[q, k, base + o - 1]).wait()
                    here[...] = (here[...].astype(F32) + part).astype(BF)
                    remote(here, slot_g.at[q, k, base + o], rs_send.at[q, k], rs_got.at[q, k, base + o], near[way]).start()

    def dring_step(o, layer, r, k):
        rows_k = pl.ds(k * half, half)
        for way, length, base in ways[k]:

            @pl.when(o < length)
            def _():
                b = coming(way, length, o)
                own = own_d.at[r, b, rows_k]
                part = got_d[b, rows_k].astype(F32) + own[...].astype(F32)

                @pl.when(o == 0)
                def _():
                    own[...] = part.astype(BF)
                    remote(own, slot_d.at[r, k, base], drs_start.at[r, k], drs_got.at[r, k, base], near[way]).start()

                @pl.when(o > 0)
                def _():
                    here = slot_d.at[r, k, base + o - 1]
                    pltpu.make_async_copy(here, here, drs_got.at[r, k, base + o - 1]).wait()
                    here[...] = (here[...].astype(F32) + part).astype(BF)
                    remote(here, slot_d.at[r, k, base + o], drs_send.at[r, k], drs_got.at[r, k, base + o], near[way]).start()

    def publish(src, dst, keep, send, got, fsend, fgot, k):
        pltpu.make_async_copy(src, dst, keep).start()
        for way, _, base in ways[k]:
            remote(src, dst, send, got.at[base], near[way]).start()
        remote(src, dst, fsend, fgot, mate).start()

    def arrived(slots, sems, starts, starting, k):
        pltpu.make_async_copy(starting, starting, starts).wait()
        first, second = (slots.at[base + length - 1] for _, length, base in ways[k])
        for (_, length, base), here in zip(ways[k], (first, second)):
            pltpu.make_async_copy(here, here, sems.at[base + length - 1]).wait()
        return first, first[...].astype(F32) + second[...].astype(F32)

    def own_step(layer, j, q, k):
        cols, outs = strip_outs(layer, j)
        here, sums = arrived(slot_g.at[q, k], rs_got.at[q, k], rs_start.at[q, k], own_g.at[j, k, pl.ds(0, 2)], k)
        part = got_g[j, k, z].astype(F32) + own_g[j, k, z].astype(F32)
        g = (sums + part).astype(BF).astype(F32)
        w1, m1, v1 = adamw(wo_g[k, layer, :, cols].astype(F32), m_g[k, layer, :, cols], v_g[k, layer, :, cols], g)
        m_g[k, layer, :, cols], v_g[k, layer, :, cols], here[...] = m1, v1, w1
        publish(
            here, outs[k].at[layer, block_of(k, z), cols], keep_w.at[q, k],
            ag_send.at[q, k], ag_got.at[q, k], fw_send.at[q, k], fw_got.at[q, k], k,
        )
        pltpu.make_async_copy(m_g.at[k, layer, :, cols], (omg_ref, omu_ref)[k].at[layer, :, cols], keep_m.at[q, k]).start()
        pltpu.make_async_copy(v_g.at[k, layer, :, cols], (ovg_ref, ovu_ref)[k].at[layer, :, cols], keep_v.at[q, k]).start()

    def down_own_step(layer, r, k):
        rows_k = pl.ds(k * half, half)
        starting = own_d.at[r, pl.ds(0, 2), rows_k]
        here, sums = arrived(slot_d.at[r, k], drs_got.at[r, k], drs_start.at[r, k], starting, k)
        part = got_d[z, rows_k].astype(F32) + own_d[r, z, rows_k].astype(F32)
        g = (sums + part).astype(BF).astype(F32)
        w1, m1, v1 = adamw(wo_d[layer, rows_k].astype(F32), m_d[layer, rows_k], v_d[layer, rows_k], g)
        m_d[layer, rows_k], v_d[layer, rows_k], here[...] = m1, v1, w1
        publish(
            here, nd_ref.at[layer, dblock_of(k, z)], dkeep_w.at[r, k],
            dag_send.at[r, k], dag_got.at[r, k], dfw_send.at[r, k], dfw_got.at[r, k], k,
        )
        pltpu.make_async_copy(m_d.at[layer, rows_k], omd_ref.at[layer, rows_k], dkeep_m.at[r, k]).start()
        pltpu.make_async_copy(v_d.at[layer, rows_k], ovd_ref.at[layer, rows_k], dkeep_v.at[r, k]).start()

    def hand_on(s, here_of, send, got, fsend, fgot, k):
        for way, length, base in ways[k]:

            @pl.when(s <= length)
            def _():
                here = here_of(going(way, s))
                pltpu.make_async_copy(here, here, got.at[base + s - 1]).wait()

                @pl.when(s < length)
                def _():
                    remote(here, here, send, got.at[base + s], near[way]).start()

                remote(here, here, fsend, fgot, mate).start()

    def gather_step(s, layer, j, q, k):
        cols, outs = strip_outs(layer, j)
        hand_on(
            s, lambda b: outs[k].at[layer, block_of(k, b), cols],
            ag_send.at[q, k], ag_got.at[q, k], fw_send.at[q, k], fw_got.at[q, k], k,
        )

    def down_gather_step(s, layer, r, k):
        hand_on(
            s, lambda b: nd_ref.at[layer, dblock_of(k, b)],
            dag_send.at[r, k], dag_got.at[r, k], dfw_send.at[r, k], dfw_got.at[r, k], k,
        )

    steps = 2 * far + 1
    per = POINTS // 2
    lags = -(-steps // per)

    def point(i, p):
        def advance(lag, k):
            g = i - lag
            r, j = g // turns, g % turns
            o = (lag - 1) * per + p // 2
            layer, q = top - r, r * STRIPS + j

            @pl.when((g >= 0) & (g <= last) & (j < STRIPS))
            def _():
                if k == 0:

                    @pl.when(o == 0)
                    def _():
                        pltpu.make_async_copy(got_g.at[j], got_g.at[j], pair_got.at[q]).wait()

                    @pl.when((o == 0) & (j == STRIPS - 1))
                    def _():
                        pltpu.make_async_copy(got_d, got_d, dpair_got.at[r]).wait()

                    @pl.when((o == far) & (g == 0))
                    def _():
                        for copy in params:
                            copy.wait()

                @pl.when(o < far)
                def _():
                    ring_step(o, layer, j, q, k)

                @pl.when(o == far)
                def _():
                    own_step(layer, j, q, k)

                @pl.when(o > far)
                def _():
                    gather_step(o - far, layer, j, q, k)

                @pl.when(j == STRIPS - 1)
                def _():
                    @pl.when(o < far)
                    def _():
                        dring_step(o, layer, r, k)

                    @pl.when(o == far)
                    def _():
                        down_own_step(layer, r, k)

                    @pl.when(o > far)
                    def _():
                        down_gather_step(o - far, layer, r, k)

                if k == 1:

                    @pl.when((o == far) & (r < layers - 1))
                    def _():
                        pl.semaphore_signal(credit, inc=1, device_id={"dp": mate}, device_id_type=MESH)

        for k in range(2):

            @pl.when(p % 2 == k)
            def _():
                def lag_step(idx, carry):
                    advance(1 + idx, k)
                    return carry

                lax.fori_loop(0, lags, lag_step, 0)

    def pair_copy(j, q):
        return remote(own_g.at[STRIPS + q % 2], got_g.at[j], pair_send.at[q], pair_got.at[q], mate)

    def dpair_copy(r):
        return remote(own_d.at[layers], got_d, dpair_send.at[r], dpair_got.at[r], mate)

    def segment(i, p):
        r, j = i // turns, i % turns
        q = r * STRIPS + j
        strip = (i <= last) & (j < STRIPS)

        @pl.when((i == 0) & (p == 0))
        def _():
            for k in (1, 2, 3):
                first[k].wait()

        @pl.when((i == turns) & (p == 0))
        def _():
            for k in range(4):
                second[k].wait()

        @pl.when(strip & (p < slabs))
        def _():
            strip_block(j, p)

        @pl.when((i == STRIPS - 1) & (p == slabs))
        def _():
            states.start()

        @pl.when((i == turns) & (p == slabs - 1))
        def _():
            second[4].wait()

        @pl.when(strip & (p == slabs - 1))
        def _():
            @pl.when(q >= 2)
            def _():
                pair_copy(j, q - 2).wait_send()

            @pl.when((r > 0) & (j == 0))
            def _():
                dpair_copy(r - 1).wait_send()

        @pl.when(strip & (p >= slabs - 1))
        def _():
            def one(e, carry):
                weight_rows(q, j, e // pieces, e % pieces)
                return carry

            ahead = p - (slabs - 1)
            lax.fori_loop(jnp.maximum(2 * ahead - 1, 0), jnp.minimum(2 * ahead + 1, 2 * pieces), one, 0)

        @pl.when(strip & (p == POINTS - 1))
        def _():
            @pl.when(r > 0)
            def _():
                pl.semaphore_wait(credit, 1)

            pair_copy(j, q).start()

            def one(e, carry):
                down_rows(r, j, e)
                return carry

            lax.fori_loop(0, pieces, one, 0)

            @pl.when(j == STRIPS - 1)
            def _():
                dpair_copy(r).start()

        @pl.when((i < last) & (j == STRIPS))
        def _():
            @pl.when(p == 0)
            def _():
                second[3].start()
                states.wait()

            def one(t, carry):
                state_block(t)
                return carry

            lax.fori_loop((p * blocks) // POINTS, ((p + 1) * blocks) // POINTS, one, 0)

            @pl.when(p == POINTS - 1)
            def _():
                for k in (0, 1, 2, 4):
                    second[k].start()

    def turn(i, carry):
        def part(p, carry):
            segment(i, p)
            point(i, p)
            return carry

        return lax.fori_loop(0, POINTS, part, carry)

    lax.fori_loop(0, last + 1 + lags, turn, 0)

    def all_of(ref, sem):
        pltpu.make_async_copy(ref, ref, sem).wait()

    def finish(q, carry):
        j = lax.rem(q, STRIPS)
        layer = top - q // STRIPS
        cols, outs = strip_outs(layer, j)

        @pl.when(q >= layers * STRIPS - 2)
        def _():
            pair_copy(j, q).wait_send()

        for k in range(2):
            all_of(slot_g.at[q, k, pl.ds(0, chips - 3)], rs_send.at[q, k])
            all_of(slot_g.at[q, k, pl.ds(0, chips - 1)], ag_send.at[q, k])
            all_of(got_g.at[j, k], fw_send.at[q, k])
            all_of(got_g.at[j, k], fw_got.at[q, k])
            all_of(slot_g.at[q, k, 0], keep_w.at[q, k])
            all_of(m_g.at[k, layer, :, cols], keep_m.at[q, k])
            all_of(v_g.at[k, layer, :, cols], keep_v.at[q, k])
        return carry

    lax.fori_loop(0, layers * STRIPS, finish, 0)
    for r in range(layers):
        layer = top - r
        if r == layers - 1:
            dpair_copy(r).wait_send()
        for k in range(2):
            part = pl.ds(k * half, half)
            all_of(slot_d.at[r, k, pl.ds(0, chips - 3)], drs_send.at[r, k])
            all_of(slot_d.at[r, k, pl.ds(0, chips - 1)], dag_send.at[r, k])
            all_of(got_d.at[:, part], dfw_send.at[r, k])
            all_of(got_d.at[:, part], dfw_got.at[r, k])
            all_of(slot_d.at[r, k, 0], dkeep_w.at[r, k])
            all_of(m_d.at[layer, part], dkeep_m.at[r, k])
            all_of(v_d.at[layer, part], dkeep_v.at[r, k])


def solution(mesh):
    n = mesh.shape["dp"]

    def body(x, dy, wg, wu, wd, mg, mu, md, vg, vu, vd):
        x, dy = x[0], dy[0]
        tokens, d = x.shape
        layers, _, ff = wg.shape
        chips, rows, drows = n // 2, d // n, ff // n
        half, width = drows // 2, ff // STRIPS
        tall, flat = jax.ShapeDtypeStruct((tokens, d), BF), jax.ShapeDtypeStruct((d, tokens), BF)
        sds = jax.ShapeDtypeStruct
        vm, sem = pltpu.VMEM, pltpu.SemaphoreType.DMA
        q, r = layers * STRIPS, layers
        scratch = [
            vm((tokens, d), BF), vm((d, tokens), BF), vm((tokens, d), BF), vm((d, tokens), BF),
            vm((d, ff), BF), vm((d, ff), BF), vm((ff, d), BF),
            vm((2, tokens, ff), BF), vm((tokens, width), BF),
            vm((STRIPS + 2, 2, chips, rows, width), BF), vm((STRIPS, 2, chips, rows, width), BF),
            vm((layers + 1, chips, drows, d), BF), vm((chips, drows, d), BF),
            vm((q, 2, chips - 1, rows, width), BF), vm((r, 2, chips - 1, half, d), BF),
            vm((2, layers, rows, ff), BF), vm((layers, drows, d), BF),
            vm((2, layers, rows, ff), F32), vm((2, layers, rows, ff), F32),
            vm((layers, drows, d), F32), vm((layers, drows, d), F32),
            sem((9,)), sem((tokens // BLOCK,)), sem((3,)), sem((9,)), sem((q,)), sem((q,)),
            sem((q, 2)), sem((q, 2)), sem((q, 2, chips - 1)), sem((q, 2)), sem((q, 2, chips - 1)), sem((q, 2)), sem((q, 2)),
            sem((q, 2)), sem((q, 2)), sem((q, 2)),
            sem((r,)), sem((r,)),
            sem((r, 2)), sem((r, 2)), sem((r, 2, chips - 1)), sem((r, 2)), sem((r, 2, chips - 1)), sem((r, 2)), sem((r, 2)),
            sem((r, 2)), sem((r, 2)), sem((r, 2)),
            pltpu.SemaphoreType.REGULAR,
        ]
        return pl.pallas_call(
            functools.partial(train, n),
            in_specs=[ANY] * 11,
            out_specs=[ANY] * 12,
            out_shape=[sds(t.shape, BF) for t in (wg, wu, wd)] + [sds(t.shape, F32) for t in (mg, mu, md, vg, vu, vd)] + [tall, tall, flat],
            scratch_shapes=scratch,
            compiler_params=pltpu.CompilerParams(
                collective_id=0, has_side_effects=True, vmem_limit_bytes=67_043_328
            ),
            name="step",
        )(x, dy, wg, wu, wd, mg, mu, md, vg, vu, vd)[:9]

    seq, whole, rows = P(("rep", "dp"), None, None), P(None, None, None), P(None, "dp", None)
    return jax.shard_map(
        body,
        mesh=mesh,
        in_specs=(seq, seq, whole, whole, whole) + (rows,) * 6,
        out_specs=(P("rep", None, None),) * 3 + (P("rep", "dp", None),) * 6,
        check_vma=False,
    )
```
